32 devices in a mesh: sub: 8 (over z, x), grp: 4 (over y, core).
Axes of the slice: x: 2, y: 2, z: 4, core: 2. Of those that a mesh axis runs over, the one named last changes fastest.
Arguments:
- solution: float32 [32, 128, 2048], P(('sub', 'grp')), may hold values from -6 to 6
- residual: float32 [32, 128, 2048], P(('sub', 'grp'))
- direction: float32 [32, 128, 2048], P(('sub', 'grp'))
- residual_product: float32 [128], replicated, may hold values from 65536 to 1310720
- neighbor_slots: int32 [32, 4], P(('sub', 'grp')), may hold values from 0 to 3, each once within a row
- coupling: bfloat16 [32, 96, 256, 128], P(('sub', 'grp')), may hold values from -0.375 to 0.375
- dirichlet_factor: bfloat16 [32, 96, 128, 128], P(('sub', 'grp')), may hold values from -0.5 to 0.5
- face_block: bfloat16 [32, 32, 128, 128], P(('sub', 'grp')), as said below
- neumann_factor: bfloat16 [32, 32, 128, 128], P(('sub', 'grp')), may hold values from -0.5 to 0.5
- primal_block: int32 [32, 128], P(('sub', 'grp')), may hold values from 0 to 31
- primal_basis: bfloat16 [32, 128, 128], P(('sub', 'grp')), may hold values from -1.5 to 1.5
- coarse_matrix: float32 [32, 9, 128, 128], P(('sub', 'grp')), may hold values from -0.17677669 to 0.17677669
- coarse_block_inverse: float32 [32, 128, 128], P(('sub', 'grp')), may hold values from -0.5 to 0.5
- coarse_pattern: int32 [32, 9], P(('sub', 'grp')), may hold values from 0 to 31, as said below
Outputs:
- new_solution: float32 [32, 128, 2048], P(('sub', 'grp'))
- new_residual: float32 [32, 128, 2048], P(('sub', 'grp'))
- new_direction: float32 [32, 128, 2048], P(('sub', 'grp'))
- new_product: float32 [128], replicated
The draws below stay inside these ranges and needn't reach their ends.
Inputs may be any that keep to these rules, and one draw needn't show every extreme that they name: `neighbor_slots`: each row orders the four local face slots: entry d is the slot of the face toward direction d (sub lower, sub upper, grp lower, grp upper). `coarse_pattern`: row t names 9 different subdomains, the first of them t itself; subdomain s lies on the device of index s along sub+grp, and every entry lies within 2 positions of row t along sub, cyclically. `face_block`: each block is symmetric with every eigenvalue at least 0.5.
All inputs are finite; a program needn't handle non-finite values.
Results may differ from the reference program's by a relative error of at most 0.0003.
Values sent between devices are 32-bit elements; how exact they have to be, the bound alone decides.
A program may use at most 128 MiB of HBM per device.

```python
import math
import jax
import jax.numpy as jnp
from jax import lax

LOAD_CASES = 128
FACE_SIZE = 1024
BLOCK_SIZE = 128
PRIMALS = 128
PATTERN_BLOCKS = 9
REACH_SUBS = 2
FACE_BLOCKS = 32
INNER_BLOCKS = 96
SUBDOMAINS = 32
N_SUB = 8
N_GRP = 4


def ramped_field(key, salt):
    full_shape = (SUBDOMAINS, LOAD_CASES, 2 * FACE_SIZE)
    base_key = jax.random.fold_in(key, salt)
    column = jnp.exp(jax.random.uniform(jax.random.fold_in(base_key, 1), (1, 1, 2 * FACE_SIZE), jnp.float32, math.log(0.3), math.log(3.0)))
    across = jnp.exp(jax.random.uniform(jax.random.fold_in(base_key, 2), (1, LOAD_CASES, 1), jnp.float32, math.log(0.6), math.log(2.0)))
    position = jnp.arange(SUBDOMAINS, dtype=jnp.float32) / (SUBDOMAINS - 1)
    values = jax.random.normal(jax.random.fold_in(base_key, 3), full_shape, jnp.float32)
    ramp_scale = jnp.exp(math.log(3.0) * position)
    return values * column * across * ramp_scale[:, None, None]


def draw_residual(key, part):
    return ramped_field(key, 11)


def draw_direction(key, part):
    return ramped_field(key, 23)


def draw_face_block(key, part):
    full_shape = (SUBDOMAINS, FACE_BLOCKS, BLOCK_SIZE, BLOCK_SIZE)
    mixing = jax.random.normal(jax.random.fold_in(key, 31), full_shape, jnp.float32)
    gram_part = jnp.einsum('sjab,sjcb->sjac', mixing, mixing) / BLOCK_SIZE
    low_end = 0.5
    high_end = 2.0
    diagonal = jnp.exp(jax.random.uniform(jax.random.fold_in(key, 32), full_shape[:3], jnp.float32, math.log(low_end), math.log(high_end)))
    return (gram_part + diagonal[..., None] * jnp.eye(BLOCK_SIZE, dtype=jnp.float32)).astype(jnp.bfloat16)


def draw_coarse_pattern(key, part):
    candidates = N_GRP * (2 * REACH_SUBS + 1) - 1
    row_ids = jnp.arange(SUBDOMAINS, dtype=jnp.int32)

    def one_row(row_id):
        shuffled = jax.random.permutation(jax.random.fold_in(jax.random.fold_in(key, 41), row_id), candidates)
        chosen = shuffled[:PATTERN_BLOCKS - 1].astype(jnp.int32)
        own_slot = REACH_SUBS * N_GRP + row_id % N_GRP
        chosen = chosen + (chosen >= own_slot).astype(jnp.int32)
        entry_sub = (row_id // N_GRP + chosen // N_GRP - REACH_SUBS) % N_SUB
        entries = entry_sub * N_GRP + chosen % N_GRP
        return jnp.concatenate([row_id[None], entries]).astype(jnp.int32)
    return jax.vmap(one_row)(row_ids)


def plant(values, key, least, largest):
    place = [jax.random.randint(jax.random.fold_in(key, axis), (), 0, length) for axis, length in enumerate(values.shape)]
    longest = values.shape.index(max(values.shape))
    beside = place[:longest] + [(place[longest] + 1) % values.shape[longest]] + place[longest + 1:]
    return values.at[tuple(place)].set(least).at[tuple(beside)].set(largest)


def level_of(rng, extent, pieces, least, largest):
    def one(dim, blocks):
        draws = jax.random.uniform(jax.random.fold_in(jax.random.fold_in(rng, 6), dim), (blocks,), jnp.float32, least / len(pieces), largest / len(pieces))
        return jnp.repeat(jnp.exp(draws), extent[dim] // blocks).reshape((-1,) + (1,) * (len(extent) - dim - 1))

    loudness = one(*pieces[0])
    for cut in pieces[1:]:
        loudness = loudness * one(*cut)
    return loudness


def noise(own_key, extent, width, bound, cuts=(), kind=jnp.bfloat16):
    values = jax.random.normal(own_key, extent, jnp.float32) * width
    if len(cuts) > 0:
        values = level_of(own_key, extent, cuts, -0.22, 0.18) * values
    return jnp.clip(values, min=-bound, max=bound).astype(kind)


def setup_inputs(seed: int = 0) -> dict:
    arg_keys = jax.random.split(jax.random.key(seed), 15)
    return {
        "solution": noise(arg_keys[0], (SUBDOMAINS, LOAD_CASES, 2 * FACE_SIZE), 1.0, 6.0, ((0, 32),), jnp.float32),
        "residual": draw_residual(jax.random.fold_in(arg_keys[14], 71), 0),
        "direction": draw_direction(jax.random.fold_in(arg_keys[14], 71), 0),
        "residual_product": jnp.clip(jnp.exp(jax.random.uniform(arg_keys[3], (LOAD_CASES,), jnp.float32, math.log(65536.0), math.log(1310720))), 65536.0, 1310720),
        "neighbor_slots": jax.vmap(lambda own: jax.random.permutation(own, 4))(jax.random.split(arg_keys[4], SUBDOMAINS)).reshape((SUBDOMAINS, 4)).astype(jnp.int32),
        "coupling": noise(arg_keys[5], (SUBDOMAINS, INNER_BLOCKS, 2 * BLOCK_SIZE, BLOCK_SIZE), (2 * BLOCK_SIZE) ** -0.5, 0.375, ((0, 32),)),
        "dirichlet_factor": noise(arg_keys[6], (SUBDOMAINS, INNER_BLOCKS, BLOCK_SIZE, BLOCK_SIZE), BLOCK_SIZE ** -0.5, 0.5, ((0, 32),)),
        "face_block": draw_face_block(jax.random.fold_in(arg_keys[14], 71), 0),
        "neumann_factor": noise(arg_keys[8], (SUBDOMAINS, FACE_BLOCKS, BLOCK_SIZE, BLOCK_SIZE), BLOCK_SIZE ** -0.5, 0.5, ((0, 32),)),
        "primal_block": plant(jax.random.randint(arg_keys[9], (SUBDOMAINS, PRIMALS), 0, FACE_BLOCKS), jax.random.fold_in(arg_keys[9], 1), 0, FACE_BLOCKS - 1).astype(jnp.int32),
        "primal_basis": noise(arg_keys[10], (SUBDOMAINS, PRIMALS, BLOCK_SIZE), (BLOCK_SIZE // 8) ** -0.5, 1.5, ((0, 32),)),
        "coarse_matrix": noise(arg_keys[11], (SUBDOMAINS, PATTERN_BLOCKS, PRIMALS, PRIMALS), (1.0 / (PATTERN_BLOCKS * PRIMALS) ** 0.5), 0.17677669, ((0, 32),), jnp.float32),
        "coarse_block_inverse": noise(arg_keys[12], (SUBDOMAINS, PRIMALS, PRIMALS), PRIMALS ** -0.5, 0.5, ((0, 32),), jnp.float32),
        "coarse_pattern": draw_coarse_pattern(jax.random.fold_in(arg_keys[14], 71), 0),
    }


highest_precision = lax.Precision.HIGHEST


def onehot_slots(neighbor_slots):
    return (neighbor_slots[:, :, None] == jnp.arange(4, dtype=jnp.int32)[None, None, :]).astype(jnp.float32)


def spread(owned_part, slot_onehot):
    face_width = owned_part.shape[2] // 2
    load_count = owned_part.shape[1]
    own_sub = owned_part[:, :, :face_width].reshape(N_SUB, N_GRP, load_count, face_width)
    own_grp = owned_part[:, :, face_width:].reshape(N_SUB, N_GRP, load_count, face_width)
    from_sub = jnp.roll(own_sub, 1, axis=0)
    from_grp = jnp.roll(own_grp, 1, axis=1)
    directed = jnp.stack([from_sub, own_sub, from_grp, own_grp], 2).reshape(SUBDOMAINS, 4, load_count, face_width)
    placed = jnp.einsum('sdk,sdlf->slkf', slot_onehot, directed, precision=highest_precision)
    return placed.reshape(SUBDOMAINS, load_count, FACE_BLOCKS, BLOCK_SIZE)


def collect(local_part, slot_onehot):
    load_count = local_part.shape[1]
    placed = local_part.reshape(SUBDOMAINS, load_count, 4, FACE_SIZE)
    directed = jnp.einsum('sdk,slkf->sdlf', slot_onehot, placed, precision=highest_precision)
    grid_form = directed.reshape(N_SUB, N_GRP, 4, load_count, FACE_SIZE)
    owned_sub = grid_form[:, :, 1] + jnp.roll(grid_form[:, :, 0], -1, axis=0)
    owned_grp = grid_form[:, :, 3] + jnp.roll(grid_form[:, :, 2], -1, axis=1)
    return jnp.concatenate([owned_sub, owned_grp], 3).reshape(SUBDOMAINS, load_count, 2 * FACE_SIZE)


def condensed(vector, couple, dirichlet, face_matrix):
    count_of_blocks = vector.shape[1]
    block_width = vector.shape[2]
    paired = jnp.concatenate([jnp.concatenate([vector, jnp.roll(vector, -(offset + 1), axis=1)], 2) for offset in range(3)], 1)
    interior = jnp.einsum('lib,ibk->lik', paired, couple, precision=highest_precision)
    middle = jnp.einsum('lik,ikm->lim', interior, dirichlet, precision=highest_precision)
    solved = jnp.einsum('lim,ikm->lik', middle, dirichlet, precision=highest_precision)
    returned = jnp.einsum('lik,ibk->lib', solved, couple, precision=highest_precision)
    result = jnp.einsum('ljb,jbk->ljk', vector, face_matrix, precision=highest_precision)
    for offset in range(3):
        portion = returned[:, offset * count_of_blocks:(offset + 1) * count_of_blocks]
        result = result + portion[:, :, :block_width] + jnp.roll(portion[:, :, block_width:], offset + 1, axis=1)
    return result


def apply_condensed(operands):
    vector, couple, dirichlet, face_matrix = operands
    return condensed(vector, couple.astype(jnp.float32), dirichlet.astype(jnp.float32), face_matrix.astype(jnp.float32))


def local_precondition(operands):
    halved, neumann, block_ids, basis = operands
    neumann = neumann.astype(jnp.float32)
    basis = basis.astype(jnp.float32)
    neumann_step = jnp.einsum('ljb,jbk->ljk', halved, neumann, precision=highest_precision)
    local_solve = jnp.einsum('ljk,jmk->ljm', neumann_step, neumann, precision=highest_precision)
    selector = (block_ids[:, None] == jnp.arange(halved.shape[1], dtype=jnp.int32)[None, :]).astype(jnp.float32)
    picked = jnp.einsum('ljb,cj->lcb', halved, selector, precision=highest_precision)
    coarse_residual = jnp.einsum('lcb,cb->lc', picked, basis, precision=highest_precision)
    return local_solve, coarse_residual


def spread_coarse(operands):
    coarse_correction, block_ids, basis = operands
    basis = basis.astype(jnp.float32)
    selector = (block_ids[:, None] == jnp.arange(FACE_BLOCKS, dtype=jnp.int32)[None, :]).astype(jnp.float32)
    weighted = coarse_correction[:, :, None] * basis[None]
    return jnp.einsum('lcb,cj->ljb', weighted, selector, precision=highest_precision)


def precondition(owned_part, slot_onehot, neumann_factor, primal_block, primal_basis, coarse_matrix, coarse_block_inverse, coarse_pattern):
    halved = spread(owned_part, slot_onehot) * 0.5
    local_solve, coarse_residual = lax.map(local_precondition, (halved, neumann_factor, primal_block, primal_basis))
    initial_step = jnp.einsum('pqe,pek->pqk', coarse_residual, coarse_block_inverse, precision=highest_precision)
    gathered = initial_step[coarse_pattern]
    adjacent_sum = jnp.einsum('skld,skde->sle', gathered, coarse_matrix, precision=highest_precision)
    coarse_correction = initial_step + jnp.einsum('iqc,icw->iqw', coarse_residual - adjacent_sum, coarse_block_inverse, precision=highest_precision)
    spread_back = lax.map(spread_coarse, (coarse_correction, primal_block, primal_basis))
    return collect(0.5 * (local_solve + spread_back), slot_onehot)


def reference(solution, residual, direction, residual_product, neighbor_slots, coupling, dirichlet_factor, face_block, neumann_factor, primal_block, primal_basis, coarse_matrix, coarse_block_inverse, coarse_pattern):
    slot_onehot = onehot_slots(neighbor_slots)
    local_image = lax.map(apply_condensed, (spread(direction, slot_onehot), coupling, dirichlet_factor, face_block))
    image = collect(local_image, slot_onehot)
    curvature = jnp.sum(direction * image, axis=(0, 2))
    step_length = residual_product / curvature
    new_solution = solution + step_length[None, :, None] * direction
    new_residual = residual - step_length[None, :, None] * image
    preconditioned = precondition(new_residual, slot_onehot, neumann_factor, primal_block, primal_basis, coarse_matrix, coarse_block_inverse, coarse_pattern)
    new_product = jnp.sum(new_residual * preconditioned, axis=(0, 2))
    step_ratio = new_product / residual_product
    new_direction = preconditioned + step_ratio[None, :, None] * direction
    return new_solution, new_residual, new_direction, new_product
```

```python
import functools

import jax
import jax.numpy as jnp
from jax import lax
from jax.experimental import pallas as pl
from jax.experimental.pallas import tpu as pltpu
from jax.sharding import PartitionSpec as P

REACH = 2
WINDOW = 2 * REACH + 1
MESH = pl.DeviceIdType.MESH
F32 = jnp.float32
BF16 = jnp.bfloat16
NN = (((1,), (0,)), ((), ()))
NT = (((1,), (1,)), ((), ()))


def split(value):
    high = value.astype(BF16)
    low = (value - high.astype(F32)).astype(BF16)
    return jnp.concatenate([high, low], 1)


def twice(value, axis):
    return jnp.concatenate([value, value], axis)


def dot(lhs, rhs, dims=NN):
    return lax.dot_general(lhs, rhs, dims, preferred_element_type=F32)


def exact(lhs, rhs):
    return lax.dot_general(
        lhs, rhs, NN, preferred_element_type=F32, precision=lax.Precision.HIGHEST
    )


def row_sums(value):
    return jnp.sum(value.T, axis=0, keepdims=True)


def as_columns(row, width):
    return jnp.broadcast_to(row, (width, row.shape[1])).T


def kernel(
    n_sub, n_grp,
    sol_h, res_h, dir_h, rp_ref, slots, coup_h, diri_h, face_h, neum_h, pb_ref, basis_h,
    cmat_h, cinv_h, pattern,
    osol, ores, odir, oprod,
    inv_s, U, R, Uhl, V, A, T, B, Y, RY, Hhl, LS, Ss, Sr, So, ST, Cw, Fd, Fb, Nf, basis,
    cmat, cinv, Wn, acc, crn, rcr, rel, Bs, RB, RC, corr, red_g, red_s, red_g2, red_s2, crs,
    stepb, csem, snd, rcv,
):
    ms = lax.axis_index("sub")
    mg = lax.axis_index("grp")
    width = basis.shape[0]
    nb = Fb.shape[0]
    fb = nb // 4
    n_q = Cw.shape[0] // nb
    counter = [0]
    pending = []

    def sub_at(offset):
        return (lax.rem(ms + offset + n_sub, n_sub), mg)

    def grp_at(offset):
        return (ms, lax.rem(mg + offset + n_grp, n_grp))

    def send(src, dst, device):
        i = counter[0]
        counter[0] += 1
        copy = pltpu.make_async_remote_copy(
            src_ref=src, dst_ref=dst, send_sem=snd.at[i], recv_sem=rcv.at[i],
            device_id=device, device_id_type=MESH,
        )
        copy.start()
        pending.append(copy)
        return copy

    def blocks(ref, d, count=fb, first=0):
        return ref.at[pl.ds(d * fb + first, count)]

    def columns(ref, half, k):
        return ref.at[0, :, pl.ds((half * fb + k) * width, width)]

    def fetch_face(hbm, half, buf, d, sem):
        for k in range(fb):
            pltpu.make_async_copy(columns(hbm, half, k), buf.at[d * fb + k], csem.at[sem]).start()

    def wait_face(buf, d, sem):
        pltpu.make_async_copy(blocks(buf, d), blocks(buf, d), csem.at[sem]).wait()

    fetch_face(dir_h, 0, U, 1, 0)
    fetch_face(dir_h, 1, U, 3, 1)
    neum_copy = pltpu.make_async_copy(neum_h.at[0], Nf, csem.at[7])
    neum_copy.start()

    barrier = pltpu.get_barrier_semaphore()
    for o in range(1, n_sub):
        pl.semaphore_signal(barrier, inc=1, device_id=sub_at(o), device_id_type=MESH)
    for o in range(1, n_grp):
        pl.semaphore_signal(barrier, inc=1, device_id=grp_at(o), device_id_type=MESH)
    weight_copies = [
        pltpu.make_async_copy(face_h.at[0], Fb, csem.at[10]),
        pltpu.make_async_copy(coup_h.at[0], Cw, csem.at[11]),
        pltpu.make_async_copy(diri_h.at[0], Fd, csem.at[12]),
    ]
    for c in weight_copies:
        c.start()
    small = [
        pltpu.make_async_copy(basis_h.at[0], basis, csem.at[4]),
        pltpu.make_async_copy(cmat_h.at[0], cmat, csem.at[5]),
        pltpu.make_async_copy(cinv_h.at[0], cinv, csem.at[6]),
    ]
    for c in small:
        c.start()
    fetch_face(res_h, 0, R, 0, 2)
    fetch_face(res_h, 1, R, 1, 3)
    fetch_face(sol_h, 0, osol, 0, 8)
    fetch_face(sol_h, 1, osol, 1, 9)

    for s in range(4):
        at = jnp.int32(0)
        for d in range(4):
            at = jnp.where(slots[0, d] == s, jnp.int32(d * fb), at)
        inv_s[s] = at
    acc[...] = jnp.zeros_like(acc)
    row = lax.broadcasted_iota(jnp.int32, (width, width), 0)
    col = lax.broadcasted_iota(jnp.int32, (width, width), 1)

    def prepare(d):
        def body(k, carry):
            Uhl[d * fb + k] = split(U[d * fb + k])
            return carry
        lax.fori_loop(0, fb, body, 0, unroll=2)

    wait_face(U, 1, 0)
    prepare(1)
    wait_face(U, 3, 1)
    prepare(3)

    neum_copy.wait()
    pairs_n = fb // 2

    def gram(d, k):
        factor = Nf[slots[0, d] * fb + k]
        return dot(factor, factor, NT)

    for side in range(2):
        def own(k, carry, side=side):
            So[side * fb + k] = gram(2 * side + 1, k)
            return carry
        lax.fori_loop(0, fb, own, 0, unroll=4)

        def other(k, carry, side=side):
            first = gram(2 * side, k)
            second = gram(2 * side, k + pairs_n)
            Ss[side, k] = jnp.where(row <= col, first, second)
            diagonal = jnp.sum(jnp.where(row == col, second, 0.0), axis=0, keepdims=True)
            Ss[side, pairs_n, pl.ds(8 * k, 8)] = jnp.broadcast_to(diagonal, (8, width))
            return carry
        lax.fori_loop(0, pairs_n, other, 0, unroll=2)

    small[0].wait()
    basis32 = basis[...].astype(F32)
    primal = pb_ref[...].astype(F32)
    for side in range(2):
        Bs[side, pl.ds(0, width)] = basis32
        shifted = primal - (slots[0, 2 * side] * fb).astype(F32)
        Bs[side, pl.ds(width, 8)] = jnp.broadcast_to(shifted, (8, width))

    pl.semaphore_wait(barrier, n_sub + n_grp - 2)
    u_sub = send(blocks(U, 1), blocks(U, 0), sub_at(1))
    u_grp = send(blocks(U, 3), blocks(U, 2), grp_at(1))
    for c in weight_copies:
        c.wait()

    inner = [(q, k) for k in range(fb) for q in range(n_q) if k + q + 1 < fb]
    outer = [(q, k) for k in range(fb) for q in range(n_q) if k + q + 1 >= fb]
    halves = 2 if len(inner) % 2 == 0 and fb % 2 == 0 else 1
    count = len(inner) // halves
    faces = fb // halves

    def chains(items, total):
        for i, (left, right, n, _) in enumerate(items):
            weight = Cw[n]
            A[i] = split(dot(
                jnp.concatenate([Uhl[left], Uhl[right]], 1),
                jnp.concatenate([twice(weight[:width], 0), twice(weight[width:], 0)], 0),
            ))
        for i, (_, _, n, _) in enumerate(items):
            t = dot(A[i], twice(Fd[n], 0))
            total = total + t * t
            T[i] = split(t)
        for i, (_, _, n, at) in enumerate(items):
            B[at] = split(dot(T[i], twice(Fd[n], 1), NT))
        return total

    def intra(d, h):
        base = d * fb
        j = slots[0, d] * fb
        total = acc[...]
        for g in range(faces):
            k = h * faces + g
            v = dot(Uhl[base + k], twice(Fb[j + k], 0))
            V[base + k] = v
            total = total + U[base + k] * v
        items = []
        for g in range(count):
            q, k = inner[g]
            if halves == 2:
                q = q + h * (inner[count + g][0] - q)
                k = k + h * (inner[count + g][1] - k)
            items.append((base + k, base + k + q + 1, q * nb + j + k, q * nb + base + k))
        acc[...] = chains(items, total)

    def intra_face(d):
        def body(h, carry):
            intra(d, h)
            return carry
        lax.fori_loop(0, halves, body, 0)

    def cross(rs):
        items = []
        for r in rs:
            s = lax.rem(slots[0, 0] + r, 4)
            left = inv_s[s]
            right = inv_s[lax.rem(s + 1, 4)]
            for q, k in outer:
                items.append((left + k, right + k + q + 1 - fb, q * nb + s * fb + k, q * nb + r * fb + k))
        acc[...] = chains(items, acc[...])

    def own_faces(i, carry):
        intra(1 + 2 * (i // halves), lax.rem(i, halves))
        return carry
    lax.fori_loop(0, 2 * halves, own_faces, 0)

    u_grp.wait_recv()
    prepare(2)
    intra_face(2)

    u_sub.wait_recv()
    b_sub = send(Bs.at[0], RB.at[0], sub_at(-1))
    b_grp = send(Bs.at[1], RB.at[1], grp_at(-1))
    prepare(0)
    intra_face(0)
    cross((3, 0))

    def returned(d, h):
        j = slots[0, d] * fb
        turn = lax.rem(slots[0, d] - slots[0, 0] + 4, 4)
        before = lax.rem(turn + 3, 4)
        for g in range(faces):
            k = h * faces + g
            lhs = []
            rhs = []
            for q in range(n_q):
                near = jnp.where(k + q + 1 < fb, d, turn) * fb + k
                back = k - q - 1
                far = jnp.where(back >= 0, d * fb + back, before * fb + back + fb)
                lhs += [B[q * nb + near], B[q * nb + far]]
                rhs += [
                    twice(Cw[q * nb + j + k, :width], 1),
                    twice(Cw[q * nb + lax.rem(j + back + nb, nb), width:], 1),
                ]
            y = dot(jnp.concatenate(lhs, 1), jnp.concatenate(rhs, 1), NT)
            Y[d * fb + k] = y + V[d * fb + k]

    def returned_face(d):
        def body(h, carry):
            returned(d, h)
            return carry
        lax.fori_loop(0, halves, body, 0)

    y_sub = []
    for h in range(halves):
        returned(0, h)
        y_sub.append(send(blocks(Y, 0, faces, h * faces), blocks(RY, 0, faces, h * faces), sub_at(-1)))

    cross((1, 2))

    def reduce_start(value, red, index, size, at):
        red[index] = value
        return [send(red.at[index], red.at[index], at(o)) for o in range(1, size)]

    def reduce_end(copies, red, size):
        for c in copies:
            c.wait_recv()
        for c in copies:
            c.wait_send()
            pending[:] = [other for other in pending if other is not c]
        total = red[0]
        for i in range(1, size):
            total = total + red[i]
        return total

    copies = reduce_start(row_sums(acc[...]), red_g, mg, n_grp, grp_at)
    returned_face(2)
    y_grp = [send(blocks(Y, 2), blocks(RY, 1), grp_at(-1))]
    s_sub = send(Ss.at[0], Sr.at[0], sub_at(-1))
    s_grp = send(Ss.at[1], Sr.at[1], grp_at(-1))
    part = reduce_end(copies, red_g, n_grp)
    copies = reduce_start(part, red_s, ms, n_sub, sub_at)
    returned_face(1)
    returned_face(3)
    curvature = reduce_end(copies, red_s, n_sub)
    rp = rp_ref[...]
    stepb[...] = as_columns(rp / curvature, width)

    wait_face(osol, 0, 8)
    wait_face(osol, 1, 9)
    for half in range(2):
        def iterate(k, carry, half=half):
            osol[half * fb + k] = osol[half * fb + k] + stepb[...] * U[(2 * half + 1) * fb + k]
            return carry
        lax.fori_loop(0, fb, iterate, 0, unroll=2)

    b_sub.wait_recv()
    b_grp.wait_recv()
    for c in small[1:3]:
        c.wait()
    wait_face(R, 0, 2)
    wait_face(R, 1, 3)
    for side in range(2):
        rel[side] = as_columns(RB[side, pl.ds(width, 1)], width)
    pbc = as_columns(primal, width)
    acc[...] = jnp.zeros_like(acc)

    def pick(j):
        return jnp.where(pbc == j.astype(F32), basis32, 0.0).astype(BF16)

    def pick_other(side, k):
        return jnp.where(rel[side] == lax.convert_element_type(k, F32), RB[side, pl.ds(0, width)], 0.0).astype(BF16)

    def residual_face(side, arrivals):
        d = 2 * side + 1
        for c in arrivals:
            c.wait_recv()
        lhs = []
        rhs = []
        for k in range(fb):
            i = side * fb + k
            new = R[i] - stepb[...] * (Y[d * fb + k] + RY[i])
            ores[i] = new
            Hhl[i] = split(new * 0.5)
            lhs.append(Hhl[i])
            rows = jnp.concatenate([pick(slots[0, d] * fb + k), pick_other(side, k)], 0)
            rhs.append(twice(rows, 1))
        both = dot(jnp.concatenate(lhs, 1), jnp.concatenate(rhs, 1), NT)
        crn[side] = both[:, width:]
        return both[:, :width]

    cr3 = residual_face(1, y_grp)
    cr_grp = send(crn.at[1], rcr.at[1], grp_at(1))
    cr1 = residual_face(0, y_sub)
    cr_sub = send(crn.at[0], rcr.at[0], sub_at(1))
    crs[...] = cr1 + cr3

    s_grp.wait_recv()
    s_sub.wait_recv()

    def join(side):
        def body(k, carry):
            packed = Sr[side, k]
            turned = packed.T
            diagonal = Sr[side, pairs_n, pl.ds(8 * k, 1)]
            first = jnp.where(row <= col, packed, turned)
            second = jnp.where(row > col, packed, jnp.where(row < col, turned, diagonal))
            ST[side * fb + k] = split(So[side * fb + k] + first)
            ST[side * fb + k + pairs_n] = split(So[side * fb + k + pairs_n] + second)
            return carry
        lax.fori_loop(0, pairs_n, body, 0, unroll=2)

    def local_face(side):
        def body(k, carry):
            i = side * fb + k
            hl = Hhl[i]
            both = ST[i]
            high = both[:, :width]
            solved = dot(
                jnp.concatenate([hl, hl[:, :width]], 1),
                jnp.concatenate([high, high, both[:, width:]], 0),
            )
            LS[i] = 0.5 * solved
            acc[...] += (0.5 * ores[i]) * solved
            return carry
        lax.fori_loop(0, fb, body, 0, unroll=4)

    join(1)
    join(0)
    cr_grp.wait_recv()
    cr_sub.wait_recv()
    cr = crs[...] + rcr[0] + rcr[1]
    crs[...] = cr
    first = exact(cr, cinv[...])

    def place(g, p):
        return Wn.at[g * WINDOW + p]

    Wn[mg * WINDOW + REACH] = first
    arrivals = {}
    for o in (1, -1, 2, -2):
        p = REACH - o
        arrivals[p] = send(place(mg, REACH), place(mg, p), sub_at(o))
    order = (REACH, REACH - 2, REACH + 2, REACH - 1, REACH + 1)
    column_copies = []
    if n_grp == 4:
        near = (ms, mg + 1 - 2 * lax.rem(mg, 2))
        far = lax.rem(mg + 2, 4)
        far_copies = {}

        def pass_on(p):
            far_copies[p] = send(place(mg, p), place(mg, p), (ms, far))
            column_copies.append(send(place(mg, p), place(mg, p), near))
        pass_on(REACH)
        local_face(1)
        local_face(0)
        for p in order[1:]:
            arrivals[p].wait_recv()
            pass_on(p)
        for p in order:
            far_copies[p].wait_recv()
            column_copies.append(send(place(far, p), place(far, p), near))
        for c in column_copies:
            c.wait_recv()
    else:
        local_face(1)
        local_face(0)
        for p in order:
            if p != REACH:
                arrivals[p].wait_recv()
            for o in range(1, n_grp):
                column_copies.append(send(place(mg, p), place(mg, p), grp_at(o)))
        for c in column_copies:
            c.wait_recv()

    chosen = []
    for k in range(cmat.shape[0]):
        entry = pattern[0, k]
        p = lax.min(lax.rem(entry // n_grp - ms + REACH + n_sub, n_sub), jnp.int32(WINDOW - 1))
        chosen.append(Wn[lax.rem(entry, n_grp) * WINDOW + p])
    adjacent = exact(
        jnp.concatenate(chosen, 1), cmat[...].reshape(cmat.shape[0] * width, width)
    )
    correction = Wn[mg * WINDOW + REACH] + exact(crs[...] - adjacent, cinv[...])
    corr[...] = correction
    c_sub = send(corr, RC.at[0], sub_at(-1))
    c_grp = send(corr, RC.at[1], grp_at(-1))
    product_row = row_sums(acc[...] + correction * crs[...])
    copies = reduce_start(product_row, red_g2, mg, n_grp, grp_at)

    corr_hl = split(correction * 0.5)

    def own_spread(side):
        def body(k, carry):
            i = side * fb + k
            rows = pick(slots[0, 2 * side + 1] * fb + k)
            LS[i] = LS[i] + dot(corr_hl, twice(rows, 0))
            return carry
        lax.fori_loop(0, fb, body, 0, unroll=4)

    own_spread(0)
    part = reduce_end(copies, red_g2, n_grp)
    copies = reduce_start(part, red_s2, ms, n_sub, sub_at)
    own_spread(1)

    def borrowed_spread(side):
        other_hl = split(RC[side] * 0.5)

        def body(k, carry):
            i = side * fb + k
            rows = pick_other(side, k)
            LS[i] = LS[i] + dot(other_hl, twice(rows, 0))
            return carry
        lax.fori_loop(0, fb, body, 0, unroll=4)

    c_grp.wait_recv()
    borrowed_spread(1)
    c_sub.wait_recv()
    borrowed_spread(0)
    product = reduce_end(copies, red_s2, n_sub)
    oprod[...] = product
    ratio = as_columns(product / rp, width)
    for half in range(2):
        def advance(k, carry, half=half):
            odir[half * fb + k] = LS[half * fb + k] + ratio * U[(2 * half + 1) * fb + k]
            return carry
        lax.fori_loop(0, fb, advance, 0, unroll=2)
    for c in pending:
        c.wait_send()


def store(sol, res, dirn, prod, osol, ores, odir, oprod, sem):
    width = sol.shape[2]
    for n, (src, dst) in enumerate(((sol, osol), (res, ores), (dirn, odir))):
        for i in range(src.shape[0]):
            pltpu.make_async_copy(src.at[i], dst.at[0, :, pl.ds(i * width, width)], sem.at[n]).start()
    oprod[...] = prod[...].reshape(oprod.shape)
    for n, src in enumerate((sol, res, dirn)):
        pltpu.make_async_copy(src, src, sem.at[n]).wait()


def shards(
    solution, residual, direction, residual_product, neighbor_slots, coupling,
    dirichlet_factor, face_block, neumann_factor, primal_block, primal_basis,
    coarse_matrix, coarse_block_inverse, coarse_pattern,
):
    n_sub = lax.axis_size("sub")
    n_grp = lax.axis_size("grp")
    loads = direction.shape[1]
    nb = face_block.shape[1]
    width = face_block.shape[2]
    fb = nb // 4
    inner = coupling.shape[1]
    copies = 8 + 4 + 2 + 2 + 4 + 3 * WINDOW + 2 * (n_sub + n_grp) + WINDOW * n_grp
    hbm = pl.BlockSpec(memory_space=pltpu.HBM)
    free = pl.BlockSpec(memory_space=pl.ANY)
    vmem = pl.BlockSpec(memory_space=pltpu.VMEM)
    smem = pl.BlockSpec(memory_space=pltpu.SMEM)

    def block(count, dtype=F32, cols=width):
        return pltpu.VMEM((count, loads, cols), dtype)

    group = 2 * inner // nb * (inner // nb + 1)
    group = max(group, fb * (inner // nb))
    packed = (2, fb // 2 + 1, width, width)
    scratch = [
        pltpu.SMEM((4,), jnp.int32),
        block(nb), block(2 * fb), block(nb, BF16, 2 * width), block(nb),
        block(group, BF16, 2 * width), block(group, BF16, 2 * width),
        block(inner, BF16, 2 * width), block(nb), block(2 * fb),
        block(2 * fb, BF16, 2 * width), block(2 * fb),
        pltpu.VMEM(packed, F32), pltpu.VMEM(packed, F32),
        pltpu.VMEM((2 * fb, width, width), F32), pltpu.VMEM((2 * fb, width, 2 * width), BF16),
        pltpu.VMEM(coupling.shape[1:], BF16), pltpu.VMEM(dirichlet_factor.shape[1:], BF16),
        pltpu.VMEM(face_block.shape[1:], BF16), pltpu.VMEM(neumann_factor.shape[1:], BF16),
        pltpu.VMEM(primal_basis.shape[1:], BF16),
        pltpu.VMEM(coarse_matrix.shape[1:], F32), pltpu.VMEM(coarse_block_inverse.shape[1:], F32),
        block(n_grp * WINDOW),
        pltpu.VMEM((loads, width), F32),
        block(2), block(2), block(2),
        pltpu.VMEM((2, width + 8, width), F32), pltpu.VMEM((2, width + 8, width), F32),
        block(2), pltpu.VMEM((loads, width), F32),
        pltpu.VMEM((n_grp, 1, loads), F32), pltpu.VMEM((n_sub, 1, loads), F32),
        pltpu.VMEM((n_grp, 1, loads), F32), pltpu.VMEM((n_sub, 1, loads), F32),
        pltpu.VMEM((loads, width), F32), pltpu.VMEM((loads, width), F32),
        pltpu.SemaphoreType.DMA((16,)),
        pltpu.SemaphoreType.DMA((copies,)), pltpu.SemaphoreType.DMA((copies,)),
    ]
    field = pltpu.VMEM((2 * fb, loads, width), F32)
    kept = pl.pallas_call(
        functools.partial(kernel, n_sub, n_grp),
        out_shape=(field, field, field, pltpu.VMEM((1, loads), F32)),
        in_specs=[hbm, hbm, hbm, vmem, smem, hbm, hbm, hbm, hbm, vmem, hbm, hbm, hbm, smem],
        out_specs=(vmem, vmem, vmem, vmem),
        scratch_shapes=scratch,
        compiler_params=pltpu.CompilerParams(
            collective_id=0, has_side_effects=True, vmem_limit_bytes=56 * 1024 * 1024
        ),
    )(
        solution, residual, direction, residual_product.reshape(1, -1), neighbor_slots,
        coupling, dirichlet_factor, face_block, neumann_factor, primal_block, primal_basis,
        coarse_matrix, coarse_block_inverse, coarse_pattern,
    )
    whole = jax.ShapeDtypeStruct(solution.shape, F32)
    return pl.pallas_call(
        store,
        out_shape=(whole, whole, whole, jax.ShapeDtypeStruct((loads,), F32)),
        in_specs=[vmem, vmem, vmem, vmem],
        out_specs=(free, free, free, vmem),
        scratch_shapes=[pltpu.SemaphoreType.DMA((3,))],
    )(*[pltpu.with_memory_space_constraint(x, pltpu.VMEM) for x in kept])


def solution(mesh):
    rows = P(("sub", "grp"))
    in_specs = (rows, rows, rows, P()) + (rows,) * 10
    out_specs = (rows, rows, rows, P())
    return jax.shard_map(shards, mesh=mesh, in_specs=in_specs, out_specs=out_specs, check_vma=False)
```

```python
import functools

import jax
import jax.numpy as jnp
from jax import lax
from jax.experimental import pallas as pl
from jax.experimental.pallas import tpu as pltpu
from jax.sharding import PartitionSpec as P

REACH = 2
WINDOW = 2 * REACH + 1
MESH = pl.DeviceIdType.MESH
F32 = jnp.float32
BF16 = jnp.bfloat16
NN = (((1,), (0,)), ((), ()))
NT = (((1,), (1,)), ((), ()))


def split(value):
    high = value.astype(BF16)
    low = (value - high.astype(F32)).astype(BF16)
    return jnp.concatenate([high, low], 1)


def twice(value, axis):
    return jnp.concatenate([value, value], axis)


def dot(lhs, rhs, dims=NN):
    return lax.dot_general(lhs, rhs, dims, preferred_element_type=F32)


def weights(value):
    high = value.astype(BF16)
    low = (value - high.astype(F32)).astype(BF16)
    return jnp.concatenate([high, high, low], 0)


def fine(value):
    high = value.astype(BF16)
    low = (value - high.astype(F32)).astype(BF16)
    return jnp.concatenate([high, low, high], 1)


def row_sums(value):
    return jnp.sum(value.T, axis=0, keepdims=True)


def as_columns(row, width):
    return jnp.broadcast_to(row, (width, row.shape[1])).T


def kernel(
    n_sub, n_grp,
    sol_h, res_h, dir_h, rp_h, slots_h, coup_h, diri_h, face_h, neum_h, pb_h, basis_h,
    cmat_h, cinv_h, pattern_h,
    osol, ores, odir, oprod,
    slots, pattern, inv_s, rp_ref, pb_ref, U, R, Uhl, V, A, T, B, Y, RY, Hhl, LS, Ss, Sr, So, ST,
    Cw, Fd, Fb, Nf, basis, cmat, cinv, cmat3, cinv3, Wn, acc, crn, rcr, rel, Bs, RB, RC, corr,
    PK, PO, red_a, red_b, crs, stepb, csem, snd, rcv,
):
    ms = lax.axis_index("sub")
    mg = lax.axis_index("grp")
    width = basis.shape[0]
    nb = Fb.shape[0]
    fb = nb // 4
    n_q = Cw.shape[0] // nb
    counter = [0]
    pending = []

    def sub_at(offset):
        return (lax.rem(ms + offset + n_sub, n_sub), mg)

    def grp_at(offset):
        return (ms, lax.rem(mg + offset + n_grp, n_grp))

    def send(src, dst, device):
        i = counter[0]
        counter[0] += 1
        copy = pltpu.make_async_remote_copy(
            src_ref=src, dst_ref=dst, send_sem=snd.at[i], recv_sem=rcv.at[i],
            device_id=device, device_id_type=MESH,
        )
        copy.start()
        pending.append(copy)
        return copy

    def blocks(ref, d, count=fb, first=0):
        return ref.at[pl.ds(d * fb + first, count)]

    def columns(ref, half, k):
        return ref.at[0, :, pl.ds((half * fb + k) * width, width)]

    def fetch_face(hbm, half, buf, d, sem):
        for k in range(fb):
            pltpu.make_async_copy(columns(hbm, half, k), buf.at[d * fb + k], csem.at[sem]).start()

    def wait_face(buf, d, sem):
        pltpu.make_async_copy(blocks(buf, d), blocks(buf, d), csem.at[sem]).wait()

    barrier = pltpu.get_barrier_semaphore()
    others = [(i, j) for i in range(n_sub) for j in range(n_grp) if i + j > 0]

    def device_at(i, j):
        return (lax.rem(ms + i, n_sub), lax.rem(mg + j, n_grp))

    tiny = [
        pltpu.make_async_copy(slots_h, slots, csem.at[13]),
        pltpu.make_async_copy(pattern_h, pattern, csem.at[14]),
        pltpu.make_async_copy(rp_h, rp_ref, csem.at[15]),
        pltpu.make_async_copy(pb_h, pb_ref, csem.at[16]),
    ]
    fetch_face(dir_h, 0, U, 1, 0)
    fetch_face(dir_h, 1, U, 3, 1)
    for i, j in others:
        pl.semaphore_signal(barrier, inc=1, device_id=device_at(i, j), device_id_type=MESH)
    tiny[0].start()
    neum_copy = pltpu.make_async_copy(neum_h.at[0], Nf, csem.at[7])
    small = [
        pltpu.make_async_copy(basis_h.at[0], basis, csem.at[4]),
        pltpu.make_async_copy(cmat_h.at[0], cmat, csem.at[5]),
        pltpu.make_async_copy(cinv_h.at[0], cinv, csem.at[6]),
    ]
    neum_copy.start()
    for c in tiny[1:]:
        c.start()
    small[0].start()
    weight_copies = [
        pltpu.make_async_copy(face_h.at[0], Fb, csem.at[10]),
        pltpu.make_async_copy(coup_h.at[0], Cw, csem.at[11]),
        pltpu.make_async_copy(diri_h.at[0], Fd, csem.at[12]),
    ]
    for c in weight_copies:
        c.start()
    for c in small[1:]:
        c.start()
    fetch_face(res_h, 0, R, 0, 2)
    fetch_face(res_h, 1, R, 1, 3)
    fetch_face(sol_h, 0, osol, 0, 8)
    fetch_face(sol_h, 1, osol, 1, 9)

    wait_face(U, 1, 0)
    wait_face(U, 3, 1)
    pl.semaphore_wait(barrier, len(others))
    u_sub = send(blocks(U, 1), blocks(U, 0), sub_at(1))
    u_grp = send(blocks(U, 3), blocks(U, 2), grp_at(1))

    def prepare(d):
        def body(k, carry):
            Uhl[d * fb + k] = split(U[d * fb + k])
            return carry
        lax.fori_loop(0, fb, body, 0, unroll=2)

    prepare(1)
    prepare(3)
    acc[...] = jnp.zeros_like(acc)
    row = lax.broadcasted_iota(jnp.int32, (width, width), 0)
    col = lax.broadcasted_iota(jnp.int32, (width, width), 1)
    for c in tiny:
        c.wait()
    for s in range(4):
        at = jnp.int32(0)
        for d in range(4):
            at = jnp.where(slots[0, d] == s, jnp.int32(d * fb), at)
        inv_s[s] = at

    small[0].wait()
    basis32 = basis[...].astype(F32)
    primal = pb_ref[...].astype(F32)
    for side in range(2):
        Bs[side, pl.ds(0, width)] = basis32
        shifted = primal - (slots[0, 2 * side] * fb).astype(F32)
        Bs[side, pl.ds(width, 8)] = jnp.broadcast_to(shifted, (8, width))

    neum_copy.wait()
    pairs_n = fb // 2

    def gram(d, k):
        factor = Nf[slots[0, d] * fb + k]
        return dot(factor, factor, NT)

    for side in range(2):
        def other(k, carry, side=side):
            first = gram(2 * side, k)
            second = gram(2 * side, k + pairs_n)
            Ss[side, k] = jnp.where(row <= col, first, second)
            diagonal = jnp.sum(jnp.where(row == col, second, 0.0), axis=0, keepdims=True)
            Ss[side, pairs_n, pl.ds(8 * k, 8)] = jnp.broadcast_to(diagonal, (8, width))
            return carry
        lax.fori_loop(0, pairs_n, other, 0, unroll=4)
    for c in weight_copies:
        c.wait()

    inner = [(q, k) for k in range(fb) for q in range(n_q) if k + q + 1 < fb]
    outer = [(q, k) for k in range(fb) for q in range(n_q) if k + q + 1 >= fb]
    halves = 2 if len(inner) % 2 == 0 and fb % 2 == 0 else 1
    count = len(inner) // halves
    faces = fb // halves

    def chains(items, total):
        for i, (left, right, n, _) in enumerate(items):
            weight = Cw[n]
            A[i] = split(dot(
                jnp.concatenate([Uhl[left], Uhl[right]], 1),
                jnp.concatenate([twice(weight[:width], 0), twice(weight[width:], 0)], 0),
            ))
        for i, (_, _, n, _) in enumerate(items):
            t = dot(A[i], twice(Fd[n], 0))
            total = total + t * t
            T[i] = split(t)
        for i, (_, _, n, at) in enumerate(items):
            B[at] = split(dot(T[i], twice(Fd[n], 1), NT))
        return total

    def intra(d, h):
        base = d * fb
        j = slots[0, d] * fb
        total = acc[...]
        for g in range(faces):
            k = h * faces + g
            v = dot(Uhl[base + k], twice(Fb[j + k], 0))
            V[base + k] = v
            total = total + U[base + k] * v
        items = []
        for g in range(count):
            q, k = inner[g]
            if halves == 2:
                q = q + h * (inner[count + g][0] - q)
                k = k + h * (inner[count + g][1] - k)
            items.append((base + k, base + k + q + 1, q * nb + j + k, q * nb + base + k))
        acc[...] = chains(items, total)

    def intra_face(d):
        def body(h, carry):
            intra(d, h)
            return carry
        lax.fori_loop(0, halves, body, 0)

    def cross(rs):
        items = []
        for r in rs:
            s = lax.rem(slots[0, 0] + r, 4)
            left = inv_s[s]
            right = inv_s[lax.rem(s + 1, 4)]
            for q, k in outer:
                items.append((left + k, right + k + q + 1 - fb, q * nb + s * fb + k, q * nb + r * fb + k))
        acc[...] = chains(items, acc[...])

    def own_faces(i, carry):
        intra(1 + 2 * (i // halves), lax.rem(i, halves))
        return carry
    lax.fori_loop(0, 2 * halves, own_faces, 0)

    u_grp.wait_recv()
    prepare(2)
    intra_face(2)

    for side in range(2):
        def own(k, carry, side=side):
            So[side * fb + k] = gram(2 * side + 1, k)
            return carry
        lax.fori_loop(0, fb, own, 0, unroll=4)
    pbc = as_columns(primal, width)
    for side in range(2):
        def keep(k, carry, side=side):
            j = slots[0, 2 * side + 1] * fb + k
            PK[side * fb + k] = jnp.where(pbc == j.astype(F32), basis32, 0.0).astype(BF16)
            return carry
        lax.fori_loop(0, fb, keep, 0, unroll=4)
    for c in small[1:]:
        c.wait()
    cinv3[...] = weights(cinv[...])

    def halve(k, carry):
        cmat3[k] = weights(cmat[k])
        return carry
    lax.fori_loop(0, cmat.shape[0], halve, 0)

    for c in (u_grp, u_sub):
        c.wait_send()
        pending[:] = [other for other in pending if other is not c]
    b_sub = send(Bs.at[0], RB.at[0], sub_at(-1))
    b_grp = send(Bs.at[1], RB.at[1], grp_at(-1))
    u_sub.wait_recv()
    prepare(0)
    intra_face(0)

    def all_cross(i, carry):
        cross((lax.rem(3 + 2 * i, 4), 2 * i))
        return carry
    lax.fori_loop(0, 2, all_cross, 0)

    me = ms * n_grp + mg

    def total_start(value, red):
        red[me] = value
        return [send(red.at[me], red.at[me], device_at(i, j)) for i, j in others]

    def total_end(copies, red):
        for c in copies:
            c.wait_recv()
        return jnp.sum(red[...], axis=0)

    copies = total_start(row_sums(acc[...]), red_a)

    def returned(d, h):
        j = slots[0, d] * fb
        turn = lax.rem(slots[0, d] - slots[0, 0] + 4, 4)
        before = lax.rem(turn + 3, 4)
        for g in range(faces):
            k = h * faces + g
            lhs = []
            rhs = []
            for q in range(n_q):
                near = jnp.where(k + q + 1 < fb, d, turn) * fb + k
                back = k - q - 1
                far = jnp.where(back >= 0, d * fb + back, before * fb + back + fb)
                lhs += [B[q * nb + near], B[q * nb + far]]
                rhs += [
                    twice(Cw[q * nb + j + k, :width], 1),
                    twice(Cw[q * nb + lax.rem(j + back + nb, nb), width:], 1),
                ]
            y = dot(jnp.concatenate(lhs, 1), jnp.concatenate(rhs, 1), NT)
            Y[d * fb + k] = y + V[d * fb + k]

    def returned_face(d):
        def body(h, carry):
            returned(d, h)
            return carry
        lax.fori_loop(0, halves, body, 0)

    y_sub = []
    for h in range(halves):
        returned(0, h)
        y_sub.append(send(blocks(Y, 0, faces, h * faces), blocks(RY, 0, faces, h * faces), sub_at(-1)))
    returned_face(2)
    y_grp = [send(blocks(Y, 2), blocks(RY, 1), grp_at(-1))]
    returned_face(1)
    b_sub.wait_recv()
    b_grp.wait_recv()
    for side in range(2):
        rel[side] = as_columns(RB[side, pl.ds(width, 1)], width)

        def keep_other(k, carry, side=side):
            rows = jnp.where(rel[side] == k.astype(F32), RB[side, pl.ds(0, width)], 0.0)
            PO[side * fb + k] = rows.astype(BF16)
            return carry
        lax.fori_loop(0, fb, keep_other, 0, unroll=4)
    wait_face(R, 0, 2)
    wait_face(R, 1, 3)

    returned_face(3)
    curvature = total_end(copies, red_a)
    rp = rp_ref[...]
    stepb[...] = as_columns(rp / curvature, width)

    def lend(side):
        lhs = []
        rhs = []
        for k in range(fb):
            i = side * fb + k
            part = R[i] - stepb[...] * Y[(2 * side + 1) * fb + k]
            R[i] = part
            lhs.append(split(part * 0.5))
            rhs.append(twice(PO[i], 1))
        crn[side] = dot(jnp.concatenate(lhs, 1), jnp.concatenate(rhs, 1), NT)

    lend(0)
    cr_sub = send(crn.at[0], rcr.at[0], sub_at(1))
    lend(1)
    cr_grp = send(crn.at[1], rcr.at[1], grp_at(1))
    s_grp = send(Ss.at[1], Sr.at[1], grp_at(-1))

    lhs = []
    rhs = []
    for d in (0, 2):
        for k in range(fb):
            j = slots[0, d] * fb + k
            rows = jnp.where(pbc == j.astype(F32), basis32, 0.0).astype(BF16)
            lhs.append(split(Y[d * fb + k] * 0.5))
            rhs.append(twice(rows, 1))
    crs[...] = -stepb[...] * dot(jnp.concatenate(lhs, 1), jnp.concatenate(rhs, 1), NT)
    wait_face(osol, 0, 8)
    wait_face(osol, 1, 9)
    for half in range(2):
        def iterate(k, carry, half=half):
            osol[half * fb + k] = osol[half * fb + k] + stepb[...] * U[(2 * half + 1) * fb + k]
            return carry
        lax.fori_loop(0, fb, iterate, 0, unroll=2)
    acc[...] = jnp.zeros_like(acc)

    def residual_face(side, arrivals):
        for c in arrivals:
            c.wait_recv()
        lhs = []
        rhs = []
        for k in range(fb):
            i = side * fb + k
            new = R[i] - stepb[...] * RY[i]
            ores[i] = new
            Hhl[i] = split(new * 0.5)
            lhs.append(Hhl[i])
            rhs.append(twice(PK[i], 1))
        return dot(jnp.concatenate(lhs, 1), jnp.concatenate(rhs, 1), NT)

    def local_face(side):
        def body(k, carry):
            i = side * fb + k
            hl = Hhl[i]
            both = ST[i]
            high = both[:, :width]
            solved = dot(
                jnp.concatenate([hl, hl[:, :width]], 1),
                jnp.concatenate([high, high, both[:, width:]], 0),
            )
            LS[i] = 0.5 * solved
            acc[...] += (0.5 * ores[i]) * solved
            return carry
        lax.fori_loop(0, fb, body, 0, unroll=4)

    def join_face(side):
        def join(k, carry):
            packed = Sr[side, k]
            turned = packed.T
            diagonal = Sr[side, pairs_n, pl.ds(8 * k, 1)]
            first = jnp.where(row <= col, packed, turned)
            second = jnp.where(row > col, packed, jnp.where(row < col, turned, diagonal))
            ST[side * fb + k] = split(So[side * fb + k] + first)
            ST[side * fb + k + pairs_n] = split(So[side * fb + k + pairs_n] + second)
            return carry
        lax.fori_loop(0, pairs_n, join, 0, unroll=2)

    crs[...] += residual_face(1, y_grp)
    s_grp.wait_recv()
    join_face(1)
    local_face(1)
    cr_grp.wait_recv()
    crs[...] += rcr[1]
    crs[...] += residual_face(0, y_sub)
    cr_sub.wait_recv()
    cr = crs[...] + rcr[0]
    crs[...] = cr
    first = dot(fine(cr), cinv3[...])

    def place(g, p):
        return Wn.at[g * WINDOW + p]

    Wn[mg * WINDOW + REACH] = first
    arrivals = {}
    for o in (1, -1, 2, -2):
        p = REACH - o
        arrivals[p] = send(place(mg, REACH), place(mg, p), sub_at(o))
    order = (REACH, REACH - 2, REACH + 2, REACH - 1, REACH + 1)
    column_copies = []
    if n_grp == 4:
        near = (ms, mg + 1 - 2 * lax.rem(mg, 2))
        far = lax.rem(mg + 2, 4)
        far_copies = {}

        def pass_on(p):
            far_copies[p] = send(place(mg, p), place(mg, p), (ms, far))
            column_copies.append(send(place(mg, p), place(mg, p), near))
        pass_on(REACH)
        for p in order[1:]:
            arrivals[p].wait_recv()
            pass_on(p)
        s_sub = send(Ss.at[0], Sr.at[0], sub_at(-1))
        for p in order:
            far_copies[p].wait_recv()
            column_copies.append(send(place(far, p), place(far, p), near))
        s_sub.wait_recv()
        join_face(0)
        local_face(0)
        for c in column_copies:
            c.wait_recv()
    else:
        for p in order:
            if p != REACH:
                arrivals[p].wait_recv()
            for o in range(1, n_grp):
                column_copies.append(send(place(mg, p), place(mg, p), grp_at(o)))
        s_sub = send(Ss.at[0], Sr.at[0], sub_at(-1))
        s_sub.wait_recv()
        join_face(0)
        local_face(0)
        for c in column_copies:
            c.wait_recv()

    chosen = []
    for k in range(cmat.shape[0]):
        entry = pattern[0, k]
        p = lax.min(lax.rem(entry // n_grp - ms + REACH + n_sub, n_sub), jnp.int32(WINDOW - 1))
        chosen.append(Wn[lax.rem(entry, n_grp) * WINDOW + p])
    adjacent = dot(
        jnp.concatenate([fine(c) for c in chosen], 1),
        cmat3[...].reshape(cmat3.shape[0] * cmat3.shape[1], width),
    )
    correction = Wn[mg * WINDOW + REACH] + dot(fine(crs[...] - adjacent), cinv3[...])
    corr[...] = correction
    c_sub = send(corr, RC.at[0], sub_at(-1))
    c_grp = send(corr, RC.at[1], grp_at(-1))
    product_row = row_sums(acc[...] + correction * crs[...])
    copies = total_start(product_row, red_b)

    corr_hl = split(correction * 0.5)
    for side in range(2):
        def own_spread(k, carry, side=side):
            i = side * fb + k
            LS[i] = LS[i] + dot(corr_hl, twice(PK[i], 0))
            return carry
        lax.fori_loop(0, fb, own_spread, 0, unroll=4)

    def borrowed_spread(side):
        other_hl = split(RC[side] * 0.5)

        def body(k, carry):
            i = side * fb + k
            LS[i] = LS[i] + dot(other_hl, twice(PO[i], 0))
            return carry
        lax.fori_loop(0, fb, body, 0, unroll=4)

    c_grp.wait_recv()
    borrowed_spread(1)
    c_sub.wait_recv()
    borrowed_spread(0)
    product = total_end(copies, red_b)
    oprod[...] = product
    ratio = as_columns(product / rp, width)
    for half in range(2):
        def advance(k, carry, half=half):
            odir[half * fb + k] = LS[half * fb + k] + ratio * U[(2 * half + 1) * fb + k]
            return carry
        lax.fori_loop(0, fb, advance, 0, unroll=2)
    for c in pending:
        c.wait_send()


def store(sol, res, dirn, prod, osol, ores, odir, oprod, sem):
    width = sol.shape[2]
    for n, (src, dst) in enumerate(((sol, osol), (res, ores), (dirn, odir))):
        for i in range(src.shape[0]):
            pltpu.make_async_copy(src.at[i], dst.at[0, :, pl.ds(i * width, width)], sem.at[n]).start()
    oprod[...] = prod[...].reshape(oprod.shape)
    for n, src in enumerate((sol, res, dirn)):
        pltpu.make_async_copy(src, src, sem.at[n]).wait()


def shards(
    solution, residual, direction, residual_product, neighbor_slots, coupling,
    dirichlet_factor, face_block, neumann_factor, primal_block, primal_basis,
    coarse_matrix, coarse_block_inverse, coarse_pattern,
):
    n_sub = lax.axis_size("sub")
    n_grp = lax.axis_size("grp")
    loads = direction.shape[1]
    nb = face_block.shape[1]
    width = face_block.shape[2]
    fb = nb // 4
    inner = coupling.shape[1]
    copies = 16 + 3 * WINDOW + 2 * n_sub * n_grp + WINDOW * n_grp
    hbm = pl.BlockSpec(memory_space=pltpu.HBM)
    free = pl.BlockSpec(memory_space=pl.ANY)
    vmem = pl.BlockSpec(memory_space=pltpu.VMEM)

    def block(count, dtype=F32, cols=width):
        return pltpu.VMEM((count, loads, cols), dtype)

    n_q = inner // nb
    group = max(n_q * (n_q + 1), fb * n_q)
    packed = (2, fb // 2 + 1, width, width)
    scratch = [
        pltpu.SMEM(neighbor_slots.shape, jnp.int32), pltpu.SMEM(coarse_pattern.shape, jnp.int32),
        pltpu.SMEM((4,), jnp.int32),
        pltpu.VMEM((1, loads), F32), pltpu.VMEM(primal_block.shape, jnp.int32),
        block(nb), block(2 * fb), block(nb, BF16, 2 * width), block(nb),
        block(group, BF16, 2 * width), block(group, BF16, 2 * width),
        block(inner, BF16, 2 * width), block(nb), block(2 * fb),
        block(2 * fb, BF16, 2 * width), block(2 * fb),
        pltpu.VMEM(packed, F32), pltpu.VMEM(packed, F32),
        pltpu.VMEM((2 * fb, width, width), F32), pltpu.VMEM((2 * fb, width, 2 * width), BF16),
        pltpu.VMEM(coupling.shape[1:], BF16), pltpu.VMEM(dirichlet_factor.shape[1:], BF16),
        pltpu.VMEM(face_block.shape[1:], BF16), pltpu.VMEM(neumann_factor.shape[1:], BF16),
        pltpu.VMEM(primal_basis.shape[1:], BF16),
        pltpu.VMEM(coarse_matrix.shape[1:], F32), pltpu.VMEM(coarse_block_inverse.shape[1:], F32),
        pltpu.VMEM((coarse_matrix.shape[1], 3 * width, width), BF16), pltpu.VMEM((3 * width, width), BF16),
        block(n_grp * WINDOW),
        pltpu.VMEM((loads, width), F32),
        block(2), block(2), block(2),
        pltpu.VMEM((2, width + 8, width), F32), pltpu.VMEM((2, width + 8, width), F32),
        block(2), pltpu.VMEM((loads, width), F32),
        pltpu.VMEM((2 * fb, width, width), BF16), pltpu.VMEM((2 * fb, width, width), BF16),
        pltpu.VMEM((n_sub * n_grp, 1, loads), F32), pltpu.VMEM((n_sub * n_grp, 1, loads), F32),
        pltpu.VMEM((loads, width), F32), pltpu.VMEM((loads, width), F32),
        pltpu.SemaphoreType.DMA((20,)),
        pltpu.SemaphoreType.DMA((copies,)), pltpu.SemaphoreType.DMA((copies,)),
    ]
    field = pltpu.VMEM((2 * fb, loads, width), F32)
    kept = pl.pallas_call(
        functools.partial(kernel, n_sub, n_grp),
        out_shape=(field, field, field, pltpu.VMEM((1, loads), F32)),
        in_specs=[hbm] * 14,
        out_specs=(vmem, vmem, vmem, vmem),
        scratch_shapes=scratch,
        compiler_params=pltpu.CompilerParams(
            collective_id=0, has_side_effects=True, vmem_limit_bytes=56 * 1024 * 1024
        ),
    )(
        solution, residual, direction, residual_product.reshape(1, -1), neighbor_slots,
        coupling, dirichlet_factor, face_block, neumann_factor, primal_block, primal_basis,
        coarse_matrix, coarse_block_inverse, coarse_pattern,
    )
    whole = jax.ShapeDtypeStruct(solution.shape, F32)
    return pl.pallas_call(
        store,
        out_shape=(whole, whole, whole, jax.ShapeDtypeStruct((loads,), F32)),
        in_specs=[vmem, vmem, vmem, vmem],
        out_specs=(free, free, free, vmem),
        scratch_shapes=[pltpu.SemaphoreType.DMA((3,))],
    )(*[pltpu.with_memory_space_constraint(x, pltpu.VMEM) for x in kept])


def solution(mesh):
    rows = P(("sub", "grp"))
    in_specs = (rows, rows, rows, P()) + (rows,) * 10
    out_specs = (rows, rows, rows, P())
    return jax.shard_map(shards, mesh=mesh, in_specs=in_specs, out_specs=out_specs, check_vma=False)
```

```python
import functools

import jax
import jax.numpy as jnp
from jax import lax
from jax.experimental import pallas as pl
from jax.experimental.pallas import tpu as pltpu
from jax.sharding import PartitionSpec as P

REACH = 2
WINDOW = 2 * REACH + 1
MESH = pl.DeviceIdType.MESH
F32 = jnp.float32
BF16 = jnp.bfloat16
NN = (((1,), (0,)), ((), ()))
NT = (((1,), (1,)), ((), ()))


def split(value):
    high = value.astype(BF16)
    low = (value - high.astype(F32)).astype(BF16)
    return jnp.concatenate([high, low], 1)


def twice(value, axis):
    return jnp.concatenate([value, value], axis)


def dot(lhs, rhs, dims=NN):
    return lax.dot_general(lhs, rhs, dims, preferred_element_type=F32)


def weights(value):
    high = value.astype(BF16)
    low = (value - high.astype(F32)).astype(BF16)
    return jnp.concatenate([high, high, low], 0)


def fine(value):
    high = value.astype(BF16)
    low = (value - high.astype(F32)).astype(BF16)
    return jnp.concatenate([high, low, high], 1)


def row_sums(value):
    return jnp.sum(value.T, axis=0, keepdims=True)


def as_columns(row, width):
    return jnp.broadcast_to(row, (width, row.shape[1])).T


def kernel(
    n_sub, n_grp,
    sol_h, res_h, dir_h, rp_h, slots_h, coup_h, diri_h, face_h, neum_h, pb_h, basis_h,
    cmat_h, cinv_h, pattern_h,
    osol, ores, odir, oprod,
    slots, pattern, inv_s, rp_ref, pb_ref, U, R, Uhl, V, A, T, B, Y, RY, Hhl, LS, Ss, Sr, So, ST,
    Cw, Fd, Fb, Nf, basis, cmat, cinv, cmat3, cinv3, Wn, acc, crn, rcr, rel, Bs, RB, RC, corr,
    PK, PO, red_a, red_b, crs, stepb, csem, snd, rcv,
):
    ms = lax.axis_index("sub")
    mg = lax.axis_index("grp")
    width = basis.shape[0]
    nb = Fb.shape[0]
    fb = nb // 4
    n_q = Cw.shape[0] // nb
    counter = [0]
    pending = []

    def sub_at(offset):
        return (lax.rem(ms + offset + n_sub, n_sub), mg)

    def grp_at(offset):
        return (ms, lax.rem(mg + offset + n_grp, n_grp))

    def send(src, dst, device):
        i = counter[0]
        counter[0] += 1
        copy = pltpu.make_async_remote_copy(
            src_ref=src, dst_ref=dst, send_sem=snd.at[i], recv_sem=rcv.at[i],
            device_id=device, device_id_type=MESH,
        )
        copy.start()
        pending.append(copy)
        return copy

    def blocks(ref, d, count=fb, first=0):
        return ref.at[pl.ds(d * fb + first, count)]

    def columns(ref, half, k):
        return ref.at[0, :, pl.ds((half * fb + k) * width, width)]

    def fetch_face(hbm, half, buf, d, sem):
        for k in range(fb):
            pltpu.make_async_copy(columns(hbm, half, k), buf.at[d * fb + k], csem.at[sem]).start()

    def wait_face(buf, d, sem):
        pltpu.make_async_copy(blocks(buf, d), blocks(buf, d), csem.at[sem]).wait()

    barrier = pltpu.get_barrier_semaphore()
    others = [(i, j) for i in range(n_sub) for j in range(n_grp) if i + j > 0]

    def device_at(i, j):
        return (lax.rem(ms + i, n_sub), lax.rem(mg + j, n_grp))

    tiny = [
        pltpu.make_async_copy(slots_h, slots, csem.at[13]),
        pltpu.make_async_copy(pattern_h, pattern, csem.at[14]),
        pltpu.make_async_copy(rp_h, rp_ref, csem.at[15]),
        pltpu.make_async_copy(pb_h, pb_ref, csem.at[16]),
    ]
    fetch_face(dir_h, 0, U, 1, 0)
    fetch_face(dir_h, 1, U, 3, 1)
    for i, j in others:
        pl.semaphore_signal(barrier, inc=1, device_id=device_at(i, j), device_id_type=MESH)
    tiny[0].start()
    neum_copy = pltpu.make_async_copy(neum_h.at[0], Nf, csem.at[7])
    small = [
        pltpu.make_async_copy(basis_h.at[0], basis, csem.at[4]),
        pltpu.make_async_copy(cmat_h.at[0], cmat, csem.at[5]),
        pltpu.make_async_copy(cinv_h.at[0], cinv, csem.at[6]),
    ]
    neum_copy.start()
    for c in tiny[1:]:
        c.start()
    small[0].start()
    weight_copies = [
        pltpu.make_async_copy(face_h.at[0], Fb, csem.at[10]),
        pltpu.make_async_copy(coup_h.at[0], Cw, csem.at[11]),
        pltpu.make_async_copy(diri_h.at[0], Fd, csem.at[12]),
    ]
    for c in weight_copies:
        c.start()
    for c in small[1:]:
        c.start()
    fetch_face(res_h, 0, R, 0, 2)
    fetch_face(res_h, 1, R, 1, 3)
    fetch_face(sol_h, 0, osol, 0, 8)
    fetch_face(sol_h, 1, osol, 1, 9)

    wait_face(U, 1, 0)
    wait_face(U, 3, 1)
    pl.semaphore_wait(barrier, len(others))
    ahead = fb - max(1, fb // 4)
    u_sub = [
        send(blocks(U, 1, ahead), blocks(U, 0, ahead), sub_at(1)),
        send(blocks(U, 1, fb - ahead, ahead), blocks(U, 0, fb - ahead, ahead), sub_at(1)),
    ]
    u_grp = send(blocks(U, 3), blocks(U, 2), grp_at(1))

    def prepare(d, first=0, last=fb):
        def body(k, carry):
            Uhl[d * fb + k] = split(U[d * fb + k])
            return carry
        lax.fori_loop(first, last, body, 0, unroll=2)

    prepare(1)
    prepare(3)
    acc[...] = jnp.zeros_like(acc)
    row = lax.broadcasted_iota(jnp.int32, (width, width), 0)
    col = lax.broadcasted_iota(jnp.int32, (width, width), 1)
    for c in tiny:
        c.wait()
    for s in range(4):
        at = jnp.int32(0)
        for d in range(4):
            at = jnp.where(slots[0, d] == s, jnp.int32(d * fb), at)
        inv_s[s] = at

    small[0].wait()
    basis32 = basis[...].astype(F32)
    primal = pb_ref[...].astype(F32)
    for side in range(2):
        Bs[side, pl.ds(0, width)] = basis32
        shifted = primal - (slots[0, 2 * side] * fb).astype(F32)
        Bs[side, pl.ds(width, 8)] = jnp.broadcast_to(shifted, (8, width))
    neum_copy.wait()
    pairs_n = fb // 2

    def gram(d, k):
        factor = Nf[slots[0, d] * fb + k]
        return dot(factor, factor, NT)

    for side in range(2):
        def other(k, carry, side=side):
            first = gram(2 * side, k)
            second = gram(2 * side, k + pairs_n)
            Ss[side, k] = jnp.where(row <= col, first, second)
            diagonal = jnp.sum(jnp.where(row == col, second, 0.0), axis=0, keepdims=True)
            Bs[side, pl.ds(width + 8 + 8 * k, 8)] = jnp.broadcast_to(diagonal, (8, width))
            return carry
        lax.fori_loop(0, pairs_n, other, 0, unroll=4)
    for c in weight_copies:
        c.wait()

    inner = [(q, k) for k in range(fb) for q in range(n_q) if k + q + 1 < fb]
    outer = [(q, k) for k in range(fb) for q in range(n_q) if k + q + 1 >= fb]
    halves = 2 if len(inner) % 2 == 0 and fb % 2 == 0 else 1
    count = len(inner) // halves
    faces = fb // halves

    def chains(items, total):
        for i, (left, right, n, _) in enumerate(items):
            weight = Cw[n]
            A[i] = split(dot(
                jnp.concatenate([Uhl[left], Uhl[right]], 1),
                jnp.concatenate([twice(weight[:width], 0), twice(weight[width:], 0)], 0),
            ))
        for i, (_, _, n, _) in enumerate(items):
            t = dot(A[i], twice(Fd[n], 0))
            total = total + t * t
            T[i] = split(t)
        for i, (_, _, n, at) in enumerate(items):
            B[at] = split(dot(T[i], twice(Fd[n], 1), NT))
        return total

    def intra(d, h):
        base = d * fb
        j = slots[0, d] * fb
        total = acc[...]
        for g in range(faces):
            k = h * faces + g
            v = dot(Uhl[base + k], twice(Fb[j + k], 0))
            V[base + k] = v
            total = total + U[base + k] * v
        items = []
        for g in range(count):
            q, k = inner[g]
            if halves == 2:
                q = q + h * (inner[count + g][0] - q)
                k = k + h * (inner[count + g][1] - k)
            items.append((base + k, base + k + q + 1, q * nb + j + k, q * nb + base + k))
        acc[...] = chains(items, total)

    def intra_face(d):
        def body(h, carry):
            intra(d, h)
            return carry
        lax.fori_loop(0, halves, body, 0)

    def boundary(r):
        s = lax.rem(slots[0, 0] + r, 4)
        left = inv_s[s]
        right = inv_s[lax.rem(s + 1, 4)]
        return [
            (left + k, right + k + q + 1 - fb, q * nb + s * fb + k, q * nb + r * fb + k)
            for q, k in outer
        ]

    def arrived(first, last, items):
        j = slots[0, 0] * fb
        total = acc[...]
        for k in range(first, last):
            v = dot(Uhl[k], twice(Fb[j + k], 0))
            V[k] = v
            total = total + U[k] * v
        within = [(q, k) for q, k in inner if first <= k + q + 1 < last]
        items = [(k, k + q + 1, q * nb + j + k, q * nb + k) for q, k in within] + items
        acc[...] = chains(items, total)

    def own_faces(i, carry):
        intra(1 + 2 * (i // halves), lax.rem(i, halves))
        return carry
    lax.fori_loop(0, 2 * halves, own_faces, 0)

    u_grp.wait_recv()
    prepare(2)
    intra_face(2)

    for side in range(2):
        def own(k, carry, side=side):
            So[side * fb + k] = gram(2 * side + 1, k)
            return carry
        lax.fori_loop(0, fb, own, 0, unroll=4)
    pbc = as_columns(primal, width)
    for side in range(2):
        def keep(k, carry, side=side):
            j = slots[0, 2 * side + 1] * fb + k
            PK[side * fb + k] = jnp.where(pbc == j.astype(F32), basis32, 0.0).astype(BF16)
            return carry
        lax.fori_loop(0, fb, keep, 0, unroll=4)
    for c in small[1:]:
        c.wait()
    cinv3[...] = weights(cinv[...])

    def halve(k, carry):
        cmat3[k] = weights(cmat[k])
        return carry
    lax.fori_loop(0, cmat.shape[0], halve, 0)

    acc[...] = chains(boundary(1) + boundary(2), acc[...])

    for c in [u_grp] + u_sub:
        c.wait_send()
        pending[:] = [other for other in pending if other is not c]
    b_sub = send(Bs.at[0], RB.at[0], sub_at(-1))
    b_grp = send(Bs.at[1], RB.at[1], grp_at(-1))
    u_sub[0].wait_recv()
    prepare(0, 0, ahead)
    arrived(0, ahead, boundary(3))
    u_sub[1].wait_recv()
    prepare(0, ahead, fb)
    arrived(ahead, fb, boundary(0))

    me = ms * n_grp + mg

    def total_copy(rows, device):
        i = counter[0]
        return pltpu.make_async_remote_copy(
            src_ref=rows, dst_ref=rows, send_sem=snd.at[i], recv_sem=rcv.at[i],
            device_id=device, device_id_type=MESH,
        )

    def total_start(value, red):
        red[me] = value
        for i, j in others:
            total_copy(red.at[me], device_at(i, j)).start()
        every = total_copy(red.at[pl.ds(0, len(others))], device_at(*others[0]))
        counter[0] += 1
        pending.append(every)
        return every

    def total_end(every, red):
        every.wait_recv()
        return jnp.sum(red[...], axis=0)

    copies = total_start(row_sums(acc[...]), red_a)

    def returned(d, h):
        j = slots[0, d] * fb
        turn = lax.rem(slots[0, d] - slots[0, 0] + 4, 4)
        before = lax.rem(turn + 3, 4)
        for g in range(faces):
            k = h * faces + g
            lhs = []
            rhs = []
            for q in range(n_q):
                near = jnp.where(k + q + 1 < fb, d, turn) * fb + k
                back = k - q - 1
                far = jnp.where(back >= 0, d * fb + back, before * fb + back + fb)
                lhs += [B[q * nb + near], B[q * nb + far]]
                rhs += [
                    twice(Cw[q * nb + j + k, :width], 1),
                    twice(Cw[q * nb + lax.rem(j + back + nb, nb), width:], 1),
                ]
            y = dot(jnp.concatenate(lhs, 1), jnp.concatenate(rhs, 1), NT)
            Y[d * fb + k] = y + V[d * fb + k]

    def returned_face(d):
        def body(h, carry):
            returned(d, h)
            return carry
        lax.fori_loop(0, halves, body, 0)

    y_sub = []
    for h in range(halves):
        returned(0, h)
        y_sub.append(send(blocks(Y, 0, faces, h * faces), blocks(RY, 0, faces, h * faces), sub_at(-1)))
    returned_face(2)
    y_grp = [send(blocks(Y, 2), blocks(RY, 1), grp_at(-1))]
    returned_face(1)
    b_sub.wait_recv()
    b_grp.wait_recv()
    for side in range(2):
        rel[side] = as_columns(RB[side, pl.ds(width, 1)], width)

        def keep_other(k, carry, side=side):
            rows = jnp.where(rel[side] == k.astype(F32), RB[side, pl.ds(0, width)], 0.0)
            PO[side * fb + k] = rows.astype(BF16)
            return carry
        lax.fori_loop(0, fb, keep_other, 0, unroll=4)
    wait_face(R, 0, 2)
    wait_face(R, 1, 3)

    returned_face(3)
    curvature = total_end(copies, red_a)
    rp = rp_ref[...]
    stepb[...] = as_columns(rp / curvature, width)

    def lend(side):
        lhs = []
        rhs = []
        for k in range(fb):
            i = side * fb + k
            part = R[i] - stepb[...] * Y[(2 * side + 1) * fb + k]
            R[i] = part
            lhs.append(split(part * 0.5))
            rhs.append(twice(PO[i], 1))
        crn[side] = dot(jnp.concatenate(lhs, 1), jnp.concatenate(rhs, 1), NT)

    lend(0)
    cr_sub = send(crn.at[0], rcr.at[0], sub_at(1))
    lend(1)
    cr_grp = send(crn.at[1], rcr.at[1], grp_at(1))
    s_grp = send(Ss.at[1], Sr.at[1], grp_at(-1))

    lhs = []
    rhs = []
    for d in (0, 2):
        for k in range(fb):
            j = slots[0, d] * fb + k
            rows = jnp.where(pbc == j.astype(F32), basis32, 0.0).astype(BF16)
            lhs.append(split(Y[d * fb + k] * 0.5))
            rhs.append(twice(rows, 1))
    crs[...] = -stepb[...] * dot(jnp.concatenate(lhs, 1), jnp.concatenate(rhs, 1), NT)
    wait_face(osol, 0, 8)
    wait_face(osol, 1, 9)
    for half in range(2):
        def iterate(k, carry, half=half):
            osol[half * fb + k] = osol[half * fb + k] + stepb[...] * U[(2 * half + 1) * fb + k]
            return carry
        lax.fori_loop(0, fb, iterate, 0, unroll=2)
    acc[...] = jnp.zeros_like(acc)

    def residual_face(side, arrivals):
        for c in arrivals:
            c.wait_recv()
        lhs = []
        rhs = []
        for k in range(fb):
            i = side * fb + k
            new = R[i] - stepb[...] * RY[i]
            ores[i] = new
            Hhl[i] = split(new * 0.5)
            lhs.append(Hhl[i])
            rhs.append(twice(PK[i], 1))
        return dot(jnp.concatenate(lhs, 1), jnp.concatenate(rhs, 1), NT)

    def local_face(side):
        def body(k, carry):
            i = side * fb + k
            hl = Hhl[i]
            both = ST[i]
            high = both[:, :width]
            solved = dot(
                jnp.concatenate([hl, hl[:, :width]], 1),
                jnp.concatenate([high, high, both[:, width:]], 0),
            )
            LS[i] = 0.5 * solved
            acc[...] += (0.5 * ores[i]) * solved
            return carry
        lax.fori_loop(0, fb, body, 0, unroll=4)

    def join_face(side):
        def join(k, carry):
            packed = Sr[side, k]
            turned = packed.T
            diagonal = RB[side, pl.ds(width + 8 + 8 * k, 1)]
            first = jnp.where(row <= col, packed, turned)
            second = jnp.where(row > col, packed, jnp.where(row < col, turned, diagonal))
            ST[side * fb + k] = split(So[side * fb + k] + first)
            ST[side * fb + k + pairs_n] = split(So[side * fb + k + pairs_n] + second)
            return carry
        lax.fori_loop(0, pairs_n, join, 0, unroll=2)

    crs[...] += residual_face(1, y_grp)
    s_grp.wait_recv()
    join_face(1)
    local_face(1)
    cr_grp.wait_recv()
    crs[...] += rcr[1]
    crs[...] += residual_face(0, y_sub)
    cr_sub.wait_recv()
    cr = crs[...] + rcr[0]
    crs[...] = cr
    first = dot(fine(cr), cinv3[...])

    pieces = 1
    rows = first.shape[0] // pieces

    def place(g, p, h):
        return Wn.at[g * WINDOW + p, pl.ds(h * rows, rows)]

    Wn[mg * WINDOW + REACH] = first
    arrivals = {}
    for h in range(pieces):
        for o in (2, -2, 1, -1):
            p = REACH - o
            arrivals[p, h] = send(place(mg, REACH, h), place(mg, p, h), sub_at(o))
    order = (REACH, REACH - 2, REACH + 2, REACH - 1, REACH + 1)
    column_copies = []
    if n_grp == 4:
        near = (ms, mg + 1 - 2 * lax.rem(mg, 2))
        far = lax.rem(mg + 2, 4)
        far_copies = {}

        def pass_on(p, h):
            far_copies[p, h] = send(place(mg, p, h), place(mg, p, h), (ms, far))
            column_copies.append(send(place(mg, p, h), place(mg, p, h), near))
        for h in range(pieces):
            pass_on(REACH, h)
        for i, p in enumerate(order[1:]):
            for h in range(pieces):
                arrivals[p, h].wait_recv()
                pass_on(p, h)
            if i == 0:
                s_sub = send(Ss.at[0], Sr.at[0], sub_at(-1))
        for p in order:
            for h in range(pieces):
                far_copies[p, h].wait_recv()
                column_copies.append(send(place(far, p, h), place(far, p, h), near))
        s_sub.wait_recv()
        join_face(0)
        local_face(0)
        for c in column_copies:
            c.wait_recv()
    else:
        for p in order:
            for h in range(pieces):
                if p != REACH:
                    arrivals[p, h].wait_recv()
                for o in range(1, n_grp):
                    column_copies.append(send(place(mg, p, h), place(mg, p, h), grp_at(o)))
        s_sub = send(Ss.at[0], Sr.at[0], sub_at(-1))
        s_sub.wait_recv()
        join_face(0)
        local_face(0)
        for c in column_copies:
            c.wait_recv()

    chosen = []
    for k in range(cmat.shape[0]):
        entry = pattern[0, k]
        p = lax.min(lax.rem(entry // n_grp - ms + REACH + n_sub, n_sub), jnp.int32(WINDOW - 1))
        chosen.append(Wn[lax.rem(entry, n_grp) * WINDOW + p])
    adjacent = dot(
        jnp.concatenate([fine(c) for c in chosen], 1),
        cmat3[...].reshape(cmat3.shape[0] * cmat3.shape[1], width),
    )
    correction = Wn[mg * WINDOW + REACH] + dot(fine(crs[...] - adjacent), cinv3[...])
    corr[...] = correction
    c_sub = send(corr, RC.at[0], sub_at(-1))
    c_grp = send(corr, RC.at[1], grp_at(-1))
    product_row = row_sums(acc[...] + correction * crs[...])
    copies = total_start(product_row, red_b)

    corr_hl = split(correction * 0.5)
    for side in range(2):
        def own_spread(k, carry, side=side):
            i = side * fb + k
            LS[i] = LS[i] + dot(corr_hl, twice(PK[i], 0))
            return carry
        lax.fori_loop(0, fb, own_spread, 0, unroll=4)

    def borrowed_spread(side):
        other_hl = split(RC[side] * 0.5)

        def body(k, carry):
            i = side * fb + k
            LS[i] = LS[i] + dot(other_hl, twice(PO[i], 0))
            return carry
        lax.fori_loop(0, fb, body, 0, unroll=4)

    c_grp.wait_recv()
    borrowed_spread(1)
    c_sub.wait_recv()
    borrowed_spread(0)
    product = total_end(copies, red_b)
    oprod[...] = product
    ratio = as_columns(product / rp, width)
    for half in range(2):
        def advance(k, carry, half=half):
            odir[half * fb + k] = LS[half * fb + k] + ratio * U[(2 * half + 1) * fb + k]
            return carry
        lax.fori_loop(0, fb, advance, 0, unroll=2)
    for c in pending:
        c.wait_send()


def store(sol, res, dirn, prod, osol, ores, odir, oprod, sem):
    width = sol.shape[2]
    for n, (src, dst) in enumerate(((sol, osol), (res, ores), (dirn, odir))):
        for i in range(src.shape[0]):
            pltpu.make_async_copy(src.at[i], dst.at[0, :, pl.ds(i * width, width)], sem.at[n]).start()
    oprod[...] = prod[...].reshape(oprod.shape)
    for n, src in enumerate((sol, res, dirn)):
        pltpu.make_async_copy(src, src, sem.at[n]).wait()


def shards(
    solution, residual, direction, residual_product, neighbor_slots, coupling,
    dirichlet_factor, face_block, neumann_factor, primal_block, primal_basis,
    coarse_matrix, coarse_block_inverse, coarse_pattern,
):
    n_sub = lax.axis_size("sub")
    n_grp = lax.axis_size("grp")
    loads = direction.shape[1]
    nb = face_block.shape[1]
    width = face_block.shape[2]
    fb = nb // 4
    inner = coupling.shape[1]
    copies = 16 + 2 * WINDOW + WINDOW * (n_grp - 1)
    hbm = pl.BlockSpec(memory_space=pltpu.HBM)
    free = pl.BlockSpec(memory_space=pl.ANY)
    vmem = pl.BlockSpec(memory_space=pltpu.VMEM)

    def block(count, dtype=F32, cols=width):
        return pltpu.VMEM((count, loads, cols), dtype)

    n_q = inner // nb
    group = max(n_q * (n_q + 1), fb * n_q)
    packed = (2, fb // 2, width, width)
    scratch = [
        pltpu.SMEM(neighbor_slots.shape, jnp.int32), pltpu.SMEM(coarse_pattern.shape, jnp.int32),
        pltpu.SMEM((4,), jnp.int32),
        pltpu.VMEM((1, loads), F32), pltpu.VMEM(primal_block.shape, jnp.int32),
        block(nb), block(2 * fb), block(nb, BF16, 2 * width), block(nb),
        block(group, BF16, 2 * width), block(group, BF16, 2 * width),
        block(inner, BF16, 2 * width), block(nb), block(2 * fb),
        block(2 * fb, BF16, 2 * width), block(2 * fb),
        pltpu.VMEM(packed, F32), pltpu.VMEM(packed, F32),
        pltpu.VMEM((2 * fb, width, width), F32), pltpu.VMEM((2 * fb, width, 2 * width), BF16),
        pltpu.VMEM(coupling.shape[1:], BF16), pltpu.VMEM(dirichlet_factor.shape[1:], BF16),
        pltpu.VMEM(face_block.shape[1:], BF16), pltpu.VMEM(neumann_factor.shape[1:], BF16),
        pltpu.VMEM(primal_basis.shape[1:], BF16),
        pltpu.VMEM(coarse_matrix.shape[1:], F32), pltpu.VMEM(coarse_block_inverse.shape[1:], F32),
        pltpu.VMEM((coarse_matrix.shape[1], 3 * width, width), BF16), pltpu.VMEM((3 * width, width), BF16),
        block(n_grp * WINDOW),
        pltpu.VMEM((loads, width), F32),
        block(2), block(2), block(2),
        pltpu.VMEM((2, width + 8 + 4 * fb, width), F32), pltpu.VMEM((2, width + 8 + 4 * fb, width), F32),
        block(2), pltpu.VMEM((loads, width), F32),
        pltpu.VMEM((2 * fb, width, width), BF16), pltpu.VMEM((2 * fb, width, width), BF16),
        pltpu.VMEM((n_sub * n_grp, 1, loads), F32), pltpu.VMEM((n_sub * n_grp, 1, loads), F32),
        pltpu.VMEM((loads, width), F32), pltpu.VMEM((loads, width), F32),
        pltpu.SemaphoreType.DMA((20,)),
        pltpu.SemaphoreType.DMA((copies,)), pltpu.SemaphoreType.DMA((copies,)),
    ]
    field = pltpu.VMEM((2 * fb, loads, width), F32)
    kept = pl.pallas_call(
        functools.partial(kernel, n_sub, n_grp),
        out_shape=(field, field, field, pltpu.VMEM((1, loads), F32)),
        in_specs=[hbm] * 14,
        out_specs=(vmem, vmem, vmem, vmem),
        scratch_shapes=scratch,
        compiler_params=pltpu.CompilerParams(
            collective_id=0, has_side_effects=True, vmem_limit_bytes=56 * 1024 * 1024
        ),
    )(
        solution, residual, direction, residual_product.reshape(1, -1), neighbor_slots,
        coupling, dirichlet_factor, face_block, neumann_factor, primal_block, primal_basis,
        coarse_matrix, coarse_block_inverse, coarse_pattern,
    )
    whole = jax.ShapeDtypeStruct(solution.shape, F32)
    return pl.pallas_call(
        store,
        out_shape=(whole, whole, whole, jax.ShapeDtypeStruct((loads,), F32)),
        in_specs=[vmem, vmem, vmem, vmem],
        out_specs=(free, free, free, vmem),
        scratch_shapes=[pltpu.SemaphoreType.DMA((3,))],
    )(*[pltpu.with_memory_space_constraint(x, pltpu.VMEM) for x in kept])


def solution(mesh):
    rows = P(("sub", "grp"))
    in_specs = (rows, rows, rows, P()) + (rows,) * 10
    out_specs = (rows, rows, rows, P())
    return jax.shard_map(shards, mesh=mesh, in_specs=in_specs, out_specs=out_specs, check_vma=False)
```

```python
import functools

import jax
import jax.numpy as jnp
from jax import lax
from jax.experimental import pallas as pl
from jax.experimental.pallas import tpu as pltpu
from jax.sharding import PartitionSpec as P

REACH = 2
WINDOW = 2 * REACH + 1
MESH = pl.DeviceIdType.MESH
F32 = jnp.float32
BF16 = jnp.bfloat16
NN = (((1,), (0,)), ((), ()))
NT = (((1,), (1,)), ((), ()))


def split(value):
    high = value.astype(BF16)
    low = (value - high.astype(F32)).astype(BF16)
    return jnp.concatenate([high, low], 1)


def twice(value, axis):
    return jnp.concatenate([value, value], axis)


def dot(lhs, rhs, dims=NN):
    return lax.dot_general(lhs, rhs, dims, preferred_element_type=F32)


def weights(value):
    high = value.astype(BF16)
    low = (value - high.astype(F32)).astype(BF16)
    return jnp.concatenate([high, high, low], 0)


def fine(value):
    high = value.astype(BF16)
    low = (value - high.astype(F32)).astype(BF16)
    return jnp.concatenate([high, low, high], 1)


def row_sums(value):
    return jnp.sum(value.T, axis=0, keepdims=True)


def as_columns(row, width):
    return jnp.broadcast_to(row, (width, row.shape[1])).T


def kernel(
    n_sub, n_grp,
    sol_h, res_h, dir_h, rp_h, slots_h, coup_h, diri_h, face_h, neum_h, pb_h, basis_h,
    cmat_h, cinv_h, pattern_h,
    osol, ores, odir, oprod,
    slots, pattern, inv_s, rp_ref, pb_ref, U, R, Uhl, V, A, T, B, Y, RY, Hhl, LS, Ss, Sr, So, ST,
    Cw, Fd, Fb, Nf, basis, cmat, cinv, cmat3, cinv3, Wn, acc, crn, rcr, rel, Bs, RB, RC, corr,
    PK, PO, red_a, red_b, crs, stepb, csem, snd, rcv,
):
    ms = lax.axis_index("sub")
    mg = lax.axis_index("grp")
    width = basis.shape[0]
    nb = Fb.shape[0]
    fb = nb // 4
    n_q = Cw.shape[0] // nb
    counter = [0]
    pending = []

    def sub_at(offset):
        return (lax.rem(ms + offset + n_sub, n_sub), mg)

    def grp_at(offset):
        return (ms, lax.rem(mg + offset + n_grp, n_grp))

    def send(src, dst, device):
        i = counter[0]
        counter[0] += 1
        copy = pltpu.make_async_remote_copy(
            src_ref=src, dst_ref=dst, send_sem=snd.at[i], recv_sem=rcv.at[i],
            device_id=device, device_id_type=MESH,
        )
        copy.start()
        pending.append(copy)
        return copy

    def blocks(ref, d, count=fb, first=0):
        return ref.at[pl.ds(d * fb + first, count)]

    def columns(ref, half, k):
        return ref.at[0, :, pl.ds((half * fb + k) * width, width)]

    def fetch_face(hbm, half, buf, d, sem):
        for k in range(fb):
            pltpu.make_async_copy(columns(hbm, half, k), buf.at[d * fb + k], csem.at[sem]).start()

    def wait_face(buf, d, sem):
        pltpu.make_async_copy(blocks(buf, d), blocks(buf, d), csem.at[sem]).wait()

    barrier = pltpu.get_barrier_semaphore()
    others = [(i, j) for i in range(n_sub) for j in range(n_grp) if i + j > 0]

    def device_at(i, j):
        return (lax.rem(ms + i, n_sub), lax.rem(mg + j, n_grp))

    tiny = [
        pltpu.make_async_copy(slots_h, slots, csem.at[13]),
        pltpu.make_async_copy(pattern_h, pattern, csem.at[14]),
        pltpu.make_async_copy(rp_h, rp_ref, csem.at[15]),
        pltpu.make_async_copy(pb_h, pb_ref, csem.at[16]),
    ]
    fetch_face(dir_h, 0, U, 1, 0)
    fetch_face(dir_h, 1, U, 3, 1)
    for i, j in others:
        pl.semaphore_signal(barrier, inc=1, device_id=device_at(i, j), device_id_type=MESH)
    tiny[0].start()
    neum_copy = pltpu.make_async_copy(neum_h.at[0], Nf, csem.at[7])
    small = [
        pltpu.make_async_copy(basis_h.at[0], basis, csem.at[4]),
        pltpu.make_async_copy(cmat_h.at[0], cmat, csem.at[5]),
        pltpu.make_async_copy(cinv_h.at[0], cinv, csem.at[6]),
    ]
    neum_copy.start()
    for c in tiny[1:]:
        c.start()
    small[0].start()
    weight_copies = [
        pltpu.make_async_copy(face_h.at[0], Fb, csem.at[10]),
        pltpu.make_async_copy(coup_h.at[0], Cw, csem.at[11]),
        pltpu.make_async_copy(diri_h.at[0], Fd, csem.at[12]),
    ]
    for c in weight_copies:
        c.start()
    for c in small[1:]:
        c.start()
    fetch_face(res_h, 0, R, 0, 2)
    fetch_face(res_h, 1, R, 1, 3)
    fetch_face(sol_h, 0, osol, 0, 8)
    fetch_face(sol_h, 1, osol, 1, 9)

    wait_face(U, 1, 0)
    wait_face(U, 3, 1)
    pl.semaphore_wait(barrier, len(others))
    ahead = fb - max(1, fb // 4)
    u_sub = [
        send(blocks(U, 1, ahead), blocks(U, 0, ahead), sub_at(1)),
        send(blocks(U, 1, fb - ahead, ahead), blocks(U, 0, fb - ahead, ahead), sub_at(1)),
    ]
    u_grp = send(blocks(U, 3), blocks(U, 2), grp_at(1))

    def prepare(d, first=0, last=fb):
        def body(k, carry):
            Uhl[d * fb + k] = split(U[d * fb + k])
            return carry
        lax.fori_loop(first, last, body, 0, unroll=2)

    prepare(1)
    prepare(3)
    acc[...] = jnp.zeros_like(acc)
    row = lax.broadcasted_iota(jnp.int32, (width, width), 0)
    col = lax.broadcasted_iota(jnp.int32, (width, width), 1)
    for c in tiny:
        c.wait()
    for s in range(4):
        at = jnp.int32(0)
        for d in range(4):
            at = jnp.where(slots[0, d] == s, jnp.int32(d * fb), at)
        inv_s[s] = at

    small[0].wait()
    basis32 = basis[...].astype(F32)
    primal = pb_ref[...].astype(F32)
    for side in range(2):
        Bs[side, pl.ds(0, width)] = basis32
        shifted = primal - (slots[0, 2 * side] * fb).astype(F32)
        Bs[side, pl.ds(width, 8)] = jnp.broadcast_to(shifted, (8, width))
    neum_copy.wait()
    pairs_n = fb // 2

    def gram(d, k):
        factor = Nf[slots[0, d] * fb + k]
        return dot(factor, factor, NT)

    for side in range(2):
        def other(k, carry, side=side):
            first = gram(2 * side, k)
            second = gram(2 * side, k + pairs_n)
            Ss[side, k] = jnp.where(row <= col, first, second)
            diagonal = jnp.sum(jnp.where(row == col, second, 0.0), axis=0, keepdims=True)
            Bs[side, pl.ds(width + 8 + 8 * k, 8)] = jnp.broadcast_to(diagonal, (8, width))
            return carry
        lax.fori_loop(0, pairs_n, other, 0, unroll=4)
    for c in weight_copies:
        c.wait()

    inner = [(q, k) for k in range(fb) for q in range(n_q) if k + q + 1 < fb]
    outer = [(q, k) for k in range(fb) for q in range(n_q) if k + q + 1 >= fb]
    halves = 2 if len(inner) % 2 == 0 and fb % 2 == 0 else 1
    count = len(inner) // halves
    faces = fb // halves

    def chains(items, total):
        for i, (left, right, n, _) in enumerate(items):
            weight = Cw[n]
            A[i] = split(dot(
                jnp.concatenate([Uhl[left], Uhl[right]], 1),
                jnp.concatenate([twice(weight[:width], 0), twice(weight[width:], 0)], 0),
            ))
        for i, (_, _, n, _) in enumerate(items):
            t = dot(A[i], twice(Fd[n], 0))
            total = total + t * t
            T[i] = split(t)
        for i, (_, _, n, at) in enumerate(items):
            B[at] = split(dot(T[i], twice(Fd[n], 1), NT))
        return total

    def intra(d, h):
        base = d * fb
        j = slots[0, d] * fb
        total = acc[...]
        for g in range(faces):
            k = h * faces + g
            v = dot(Uhl[base + k], twice(Fb[j + k], 0))
            V[base + k] = v
            total = total + U[base + k] * v
        items = []
        for g in range(count):
            q, k = inner[g]
            if halves == 2:
                q = q + h * (inner[count + g][0] - q)
                k = k + h * (inner[count + g][1] - k)
            items.append((base + k, base + k + q + 1, q * nb + j + k, q * nb + base + k))
        acc[...] = chains(items, total)

    def intra_face(d):
        def body(h, carry):
            intra(d, h)
            return carry
        lax.fori_loop(0, halves, body, 0)

    def boundary(r):
        s = lax.rem(slots[0, 0] + r, 4)
        left = inv_s[s]
        right = inv_s[lax.rem(s + 1, 4)]
        return [
            (left + k, right + k + q + 1 - fb, q * nb + s * fb + k, q * nb + r * fb + k)
            for q, k in outer
        ]

    def arrived(first, last, items):
        j = slots[0, 0] * fb
        total = acc[...]
        for k in range(first, last):
            v = dot(Uhl[k], twice(Fb[j + k], 0))
            V[k] = v
            total = total + U[k] * v
        within = [(q, k) for q, k in inner if first <= k + q + 1 < last]
        items = [(k, k + q + 1, q * nb + j + k, q * nb + k) for q, k in within] + items
        acc[...] = chains(items, total)

    def own_faces(i, carry):
        intra(1 + 2 * (i // halves), lax.rem(i, halves))
        return carry
    lax.fori_loop(0, 2 * halves, own_faces, 0)

    u_grp.wait_recv()
    prepare(2)
    intra_face(2)

    for side in range(2):
        def own(k, carry, side=side):
            So[side * fb + k] = gram(2 * side + 1, k)
            return carry
        lax.fori_loop(0, fb, own, 0, unroll=4)
    pbc = as_columns(primal, width)
    for side in range(2):
        def keep(k, carry, side=side):
            j = slots[0, 2 * side + 1] * fb + k
            PK[side * fb + k] = jnp.where(pbc == j.astype(F32), basis32, 0.0).astype(BF16)
            return carry
        lax.fori_loop(0, fb, keep, 0, unroll=4)
    for c in small[1:]:
        c.wait()
    cinv3[...] = weights(cinv[...])

    def halve(k, carry):
        cmat3[k] = weights(cmat[k])
        return carry
    lax.fori_loop(0, cmat.shape[0], halve, 0)

    acc[...] = chains(boundary(1) + boundary(2), acc[...])

    for c in [u_grp] + u_sub:
        c.wait_send()
        pending[:] = [other for other in pending if other is not c]
    b_sub = send(Bs.at[0], RB.at[0], sub_at(-1))
    b_grp = send(Bs.at[1], RB.at[1], grp_at(-1))
    u_sub[0].wait_recv()
    prepare(0, 0, ahead)
    arrived(0, ahead, boundary(3))
    u_sub[1].wait_recv()
    prepare(0, ahead, fb)
    arrived(ahead, fb, boundary(0))

    me = ms * n_grp + mg

    def total_copy(rows, device):
        i = counter[0]
        return pltpu.make_async_remote_copy(
            src_ref=rows, dst_ref=rows, send_sem=snd.at[i], recv_sem=rcv.at[i],
            device_id=device, device_id_type=MESH,
        )

    def total_start(value, red):
        red[me] = value
        for i, j in others:
            total_copy(red.at[me], device_at(i, j)).start()
        every = total_copy(red.at[pl.ds(0, len(others))], device_at(*others[0]))
        counter[0] += 1
        pending.append(every)
        return every

    def total_end(every, red):
        every.wait_recv()
        return jnp.sum(red[...], axis=0)

    copies = total_start(row_sums(acc[...]), red_a)

    def returned(d, h):
        j = slots[0, d] * fb
        turn = lax.rem(slots[0, d] - slots[0, 0] + 4, 4)
        before = lax.rem(turn + 3, 4)
        for g in range(faces):
            k = h * faces + g
            lhs = []
            rhs = []
            for q in range(n_q):
                near = jnp.where(k + q + 1 < fb, d, turn) * fb + k
                back = k - q - 1
                far = jnp.where(back >= 0, d * fb + back, before * fb + back + fb)
                lhs += [B[q * nb + near], B[q * nb + far]]
                rhs += [
                    twice(Cw[q * nb + j + k, :width], 1),
                    twice(Cw[q * nb + lax.rem(j + back + nb, nb), width:], 1),
                ]
            y = dot(jnp.concatenate(lhs, 1), jnp.concatenate(rhs, 1), NT)
            Y[d * fb + k] = y + V[d * fb + k]

    def returned_face(d):
        def body(h, carry):
            returned(d, h)
            return carry
        lax.fori_loop(0, halves, body, 0)

    y_sub = []
    for h in range(halves):
        returned(0, h)
        y_sub.append(send(blocks(Y, 0, faces, h * faces), blocks(RY, 0, faces, h * faces), sub_at(-1)))
    returned_face(2)
    y_grp = [send(blocks(Y, 2), blocks(RY, 1), grp_at(-1))]
    returned_face(1)
    b_sub.wait_recv()
    b_grp.wait_recv()
    for side in range(2):
        rel[side] = as_columns(RB[side, pl.ds(width, 1)], width)

        def keep_other(k, carry, side=side):
            rows = jnp.where(rel[side] == k.astype(F32), RB[side, pl.ds(0, width)], 0.0)
            PO[side * fb + k] = rows.astype(BF16)
            return carry
        lax.fori_loop(0, fb, keep_other, 0, unroll=4)
    wait_face(R, 0, 2)
    wait_face(R, 1, 3)

    returned_face(3)
    curvature = total_end(copies, red_a)
    rp = rp_ref[...]
    stepb[...] = as_columns(rp / curvature, width)

    def lend(side):
        lhs = []
        rhs = []
        for k in range(fb):
            i = side * fb + k
            part = R[i] - stepb[...] * Y[(2 * side + 1) * fb + k]
            R[i] = part
            lhs.append(split(part * 0.5))
            rhs.append(twice(PO[i], 1))
        crn[side] = dot(jnp.concatenate(lhs, 1), jnp.concatenate(rhs, 1), NT)

    lend(0)
    cr_sub = send(crn.at[0], rcr.at[0], sub_at(1))
    lend(1)
    cr_grp = send(crn.at[1], rcr.at[1], grp_at(1))
    s_grp = send(Ss.at[1], Sr.at[1], grp_at(-1))

    lhs = []
    rhs = []
    for d in (0, 2):
        for k in range(fb):
            j = slots[0, d] * fb + k
            rows = jnp.where(pbc == j.astype(F32), basis32, 0.0).astype(BF16)
            lhs.append(split(Y[d * fb + k] * 0.5))
            rhs.append(twice(rows, 1))
    crs[...] = -stepb[...] * dot(jnp.concatenate(lhs, 1), jnp.concatenate(rhs, 1), NT)
    wait_face(osol, 0, 8)
    wait_face(osol, 1, 9)
    for half in range(2):
        def iterate(k, carry, half=half):
            osol[half * fb + k] = osol[half * fb + k] + stepb[...] * U[(2 * half + 1) * fb + k]
            return carry
        lax.fori_loop(0, fb, iterate, 0, unroll=2)
    acc[...] = jnp.zeros_like(acc)

    def residual_face(side, arrivals):
        for c in arrivals:
            c.wait_recv()
        lhs = []
        rhs = []
        for k in range(fb):
            i = side * fb + k
            new = R[i] - stepb[...] * RY[i]
            ores[i] = new
            Hhl[i] = split(new * 0.5)
            lhs.append(Hhl[i])
            rhs.append(twice(PK[i], 1))
        return dot(jnp.concatenate(lhs, 1), jnp.concatenate(rhs, 1), NT)

    def local_face(side):
        def body(k, carry):
            i = side * fb + k
            hl = Hhl[i]
            both = ST[i]
            high = both[:, :width]
            solved = dot(
                jnp.concatenate([hl, hl[:, :width]], 1),
                jnp.concatenate([high, high, both[:, width:]], 0),
            )
            LS[i] = 0.5 * solved
            acc[...] += (0.5 * ores[i]) * solved
            return carry
        lax.fori_loop(0, fb, body, 0, unroll=4)

    def join_face(side):
        def join(k, carry):
            packed = Sr[side, k]
            turned = packed.T
            diagonal = RB[side, pl.ds(width + 8 + 8 * k, 1)]
            first = jnp.where(row <= col, packed, turned)
            second = jnp.where(row > col, packed, jnp.where(row < col, turned, diagonal))
            ST[side * fb + k] = split(So[side * fb + k] + first)
            ST[side * fb + k + pairs_n] = split(So[side * fb + k + pairs_n] + second)
            return carry
        lax.fori_loop(0, pairs_n, join, 0, unroll=2)

    crs[...] += residual_face(1, y_grp)
    s_grp.wait_recv()
    join_face(1)
    local_face(1)
    cr_grp.wait_recv()
    crs[...] += rcr[1]
    crs[...] += residual_face(0, y_sub)
    cr_sub.wait_recv()
    cr = crs[...] + rcr[0]
    crs[...] = cr
    first = dot(fine(cr), cinv3[...])

    pieces = 1
    rows = first.shape[0] // pieces

    def place(g, p, h):
        return Wn.at[g * WINDOW + p, pl.ds(h * rows, rows)]

    Wn[mg * WINDOW + REACH] = first
    arrivals = {}
    for h in range(pieces):
        for o in (2, -2, 1, -1):
            p = REACH - o
            arrivals[p, h] = send(place(mg, REACH, h), place(mg, p, h), sub_at(o))
    order = (REACH, REACH - 2, REACH + 2, REACH - 1, REACH + 1)
    column_copies = []
    if n_grp == 4:
        near = (ms, mg + 1 - 2 * lax.rem(mg, 2))
        far = lax.rem(mg + 2, 4)
        far_copies = {}

        def pass_on(p, h):
            far_copies[p, h] = send(place(mg, p, h), place(mg, p, h), (ms, far))
            column_copies.append(send(place(mg, p, h), place(mg, p, h), near))
        for h in range(pieces):
            pass_on(REACH, h)
        for i, p in enumerate(order[1:]):
            for h in range(pieces):
                arrivals[p, h].wait_recv()
                pass_on(p, h)
            if i == 0:
                s_sub = send(Ss.at[0], Sr.at[0], sub_at(-1))
        for p in order:
            for h in range(pieces):
                far_copies[p, h].wait_recv()
                column_copies.append(send(place(far, p, h), place(far, p, h), near))
        for c in column_copies:
            c.wait_recv()
    else:
        for p in order:
            for h in range(pieces):
                if p != REACH:
                    arrivals[p, h].wait_recv()
                for o in range(1, n_grp):
                    column_copies.append(send(place(mg, p, h), place(mg, p, h), grp_at(o)))
        s_sub = send(Ss.at[0], Sr.at[0], sub_at(-1))
        for c in column_copies:
            c.wait_recv()

    chosen = []
    for k in range(cmat.shape[0]):
        entry = pattern[0, k]
        p = lax.min(lax.rem(entry // n_grp - ms + REACH + n_sub, n_sub), jnp.int32(WINDOW - 1))
        chosen.append(Wn[lax.rem(entry, n_grp) * WINDOW + p])
    adjacent = dot(
        jnp.concatenate([fine(c) for c in chosen], 1),
        cmat3[...].reshape(cmat3.shape[0] * cmat3.shape[1], width),
    )
    correction = Wn[mg * WINDOW + REACH] + dot(fine(crs[...] - adjacent), cinv3[...])
    corr[...] = correction
    c_sub = send(corr, RC.at[0], sub_at(-1))
    c_grp = send(corr, RC.at[1], grp_at(-1))
    s_sub.wait_recv()
    join_face(0)
    local_face(0)
    product_row = row_sums(acc[...] + correction * crs[...])
    copies = total_start(product_row, red_b)

    corr_hl = split(correction * 0.5)
    for side in range(2):
        def own_spread(k, carry, side=side):
            i = side * fb + k
            LS[i] = LS[i] + dot(corr_hl, twice(PK[i], 0))
            return carry
        lax.fori_loop(0, fb, own_spread, 0, unroll=4)

    def borrowed_spread(side):
        other_hl = split(RC[side] * 0.5)

        def body(k, carry):
            i = side * fb + k
            LS[i] = LS[i] + dot(other_hl, twice(PO[i], 0))
            return carry
        lax.fori_loop(0, fb, body, 0, unroll=4)

    c_grp.wait_recv()
    borrowed_spread(1)
    c_sub.wait_recv()
    borrowed_spread(0)
    product = total_end(copies, red_b)
    oprod[...] = product
    ratio = as_columns(product / rp, width)
    for half in range(2):
        def advance(k, carry, half=half):
            odir[half * fb + k] = LS[half * fb + k] + ratio * U[(2 * half + 1) * fb + k]
            return carry
        lax.fori_loop(0, fb, advance, 0, unroll=2)
    for c in pending:
        c.wait_send()


def store(sol, res, dirn, prod, osol, ores, odir, oprod, sem):
    width = sol.shape[2]
    for n, (src, dst) in enumerate(((sol, osol), (res, ores), (dirn, odir))):
        for i in range(src.shape[0]):
            pltpu.make_async_copy(src.at[i], dst.at[0, :, pl.ds(i * width, width)], sem.at[n]).start()
    oprod[...] = prod[...].reshape(oprod.shape)
    for n, src in enumerate((sol, res, dirn)):
        pltpu.make_async_copy(src, src, sem.at[n]).wait()


def shards(
    solution, residual, direction, residual_product, neighbor_slots, coupling,
    dirichlet_factor, face_block, neumann_factor, primal_block, primal_basis,
    coarse_matrix, coarse_block_inverse, coarse_pattern,
):
    n_sub = lax.axis_size("sub")
    n_grp = lax.axis_size("grp")
    loads = direction.shape[1]
    nb = face_block.shape[1]
    width = face_block.shape[2]
    fb = nb // 4
    inner = coupling.shape[1]
    copies = 16 + 2 * WINDOW + WINDOW * (n_grp - 1)
    hbm = pl.BlockSpec(memory_space=pltpu.HBM)
    free = pl.BlockSpec(memory_space=pl.ANY)
    vmem = pl.BlockSpec(memory_space=pltpu.VMEM)

    def block(count, dtype=F32, cols=width):
        return pltpu.VMEM((count, loads, cols), dtype)

    n_q = inner // nb
    group = max(n_q * (n_q + 1), fb * n_q)
    packed = (2, fb // 2, width, width)
    scratch = [
        pltpu.SMEM(neighbor_slots.shape, jnp.int32), pltpu.SMEM(coarse_pattern.shape, jnp.int32),
        pltpu.SMEM((4,), jnp.int32),
        pltpu.VMEM((1, loads), F32), pltpu.VMEM(primal_block.shape, jnp.int32),
        block(nb), block(2 * fb), block(nb, BF16, 2 * width), block(nb),
        block(group, BF16, 2 * width), block(group, BF16, 2 * width),
        block(inner, BF16, 2 * width), block(nb), block(2 * fb),
        block(2 * fb, BF16, 2 * width), block(2 * fb),
        pltpu.VMEM(packed, F32), pltpu.VMEM(packed, F32),
        pltpu.VMEM((2 * fb, width, width), F32), pltpu.VMEM((2 * fb, width, 2 * width), BF16),
        pltpu.VMEM(coupling.shape[1:], BF16), pltpu.VMEM(dirichlet_factor.shape[1:], BF16),
        pltpu.VMEM(face_block.shape[1:], BF16), pltpu.VMEM(neumann_factor.shape[1:], BF16),
        pltpu.VMEM(primal_basis.shape[1:], BF16),
        pltpu.VMEM(coarse_matrix.shape[1:], F32), pltpu.VMEM(coarse_block_inverse.shape[1:], F32),
        pltpu.VMEM((coarse_matrix.shape[1], 3 * width, width), BF16), pltpu.VMEM((3 * width, width), BF16),
        block(n_grp * WINDOW),
        pltpu.VMEM((loads, width), F32),
        block(2), block(2), block(2),
        pltpu.VMEM((2, width + 8 + 4 * fb, width), F32), pltpu.VMEM((2, width + 8 + 4 * fb, width), F32),
        block(2), pltpu.VMEM((loads, width), F32),
        pltpu.VMEM((2 * fb, width, width), BF16), pltpu.VMEM((2 * fb, width, width), BF16),
        pltpu.VMEM((n_sub * n_grp, 1, loads), F32), pltpu.VMEM((n_sub * n_grp, 1, loads), F32),
        pltpu.VMEM((loads, width), F32), pltpu.VMEM((loads, width), F32),
        pltpu.SemaphoreType.DMA((20,)),
        pltpu.SemaphoreType.DMA((copies,)), pltpu.SemaphoreType.DMA((copies,)),
    ]
    field = pltpu.VMEM((2 * fb, loads, width), F32)
    kept = pl.pallas_call(
        functools.partial(kernel, n_sub, n_grp),
        out_shape=(field, field, field, pltpu.VMEM((1, loads), F32)),
        in_specs=[hbm] * 14,
        out_specs=(vmem, vmem, vmem, vmem),
        scratch_shapes=scratch,
        compiler_params=pltpu.CompilerParams(
            collective_id=0, has_side_effects=True, vmem_limit_bytes=56 * 1024 * 1024
        ),
    )(
        solution, residual, direction, residual_product.reshape(1, -1), neighbor_slots,
        coupling, dirichlet_factor, face_block, neumann_factor, primal_block, primal_basis,
        coarse_matrix, coarse_block_inverse, coarse_pattern,
    )
    whole = jax.ShapeDtypeStruct(solution.shape, F32)
    return pl.pallas_call(
        store,
        out_shape=(whole, whole, whole, jax.ShapeDtypeStruct((loads,), F32)),
        in_specs=[vmem, vmem, vmem, vmem],
        out_specs=(free, free, free, vmem),
        scratch_shapes=[pltpu.SemaphoreType.DMA((3,))],
    )(*[pltpu.with_memory_space_constraint(x, pltpu.VMEM) for x in kept])


def solution(mesh):
    rows = P(("sub", "grp"))
    in_specs = (rows, rows, rows, P()) + (rows,) * 10
    out_specs = (rows, rows, rows, P())
    return jax.shard_map(shards, mesh=mesh, in_specs=in_specs, out_specs=out_specs, check_vma=False)
```
